32 devices in a mesh: dp: 1 (over z), vp: 32 (over y, x, core).
Axes of the slice: x: 4, y: 4, z: 1, core: 2. Of those that a mesh axis runs over, the one named last changes fastest.
The devices are a block of a 4x4x8 slice.
Arguments:
- hidden: bfloat16 [384, 5120], P('dp')
- w_head: bfloat16 [5120, 131072], P(None, 'vp')
- inv_temp: float32 [384], P('dp')
- target_ids: int32 [384], P('dp')
Outputs:
- output 1: float32 [384, 131072], P(('dp', 'vp'))
- output 2: float32 [384], P('dp')
All inputs are finite; a program needn't handle non-finite values.
Results may differ from the reference program's by a relative error of at most 0.001.
Values are sent between devices in bfloat16 or wider.
A program may use at most 768 MiB of HBM per device.

```python
import math
import jax
import jax.numpy as jnp
from jax import lax

BATCH = 384
HIDDEN = 5120
VOCAB = 131072
W_ROW_BLOCK = 256


def draw_head(key, direction, profile):
    num_blocks = HIDDEN // W_ROW_BLOCK
    dir_blocks = direction.reshape(num_blocks, W_ROW_BLOCK)

    def one_block(block_args):
        block_idx, dir_rows = block_args
        noise_rows = jax.random.normal(jax.random.fold_in(key, block_idx), (W_ROW_BLOCK, VOCAB), jnp.float32)
        head_rows = (noise_rows + dir_rows[:, None] * profile[None, :]) * (HIDDEN ** -0.5)
        return head_rows.astype(jnp.bfloat16)

    blocks = lax.map(one_block, (jnp.arange(num_blocks), dir_blocks))
    return blocks.reshape(HIDDEN, VOCAB)


def setup_inputs(seed: int = 0, part: int = 0) -> dict:
    base_key = jax.random.key(seed)
    shared_key = jax.random.fold_in(base_key, 1)
    part_key = jax.random.fold_in(jax.random.fold_in(base_key, 2), part)
    key_dir, key_head = jax.random.split(shared_key)
    key_hid, key_gain, key_temp, key_ids = jax.random.split(part_key, 4)
    direction = jax.random.normal(key_dir, (HIDDEN,), jnp.float32)
    vocab_pos = jnp.arange(VOCAB, dtype=jnp.float32) / VOCAB
    profile = 1.5 * jnp.exp(-8.0 * vocab_pos)
    w_head = draw_head(key_head, direction, profile)
    row_gain = 2.0 + 0.5 * jax.random.normal(key_gain, (BATCH, 1), jnp.float32)
    hidden = jax.random.normal(key_hid, (BATCH, HIDDEN), jnp.float32) + row_gain * direction[None, :] * (HIDDEN ** -0.5)
    row_pos = jnp.arange(BATCH)
    log_temp = jax.random.uniform(key_temp, (BATCH,), jnp.float32, minval=math.log(0.5), maxval=math.log(32.0))
    inv_temp = jnp.where(row_pos == 0, 32.0, jnp.exp(log_temp))
    target_ids = jax.random.randint(key_ids, (BATCH,), 0, VOCAB, dtype=jnp.int32)
    target_ids = jnp.where(row_pos == 1, VOCAB - 1, target_ids)
    return {"hidden": hidden.astype(jnp.bfloat16), "w_head": w_head, "inv_temp": inv_temp, "target_ids": target_ids}


def reference(hidden, w_head, inv_temp, target_ids):
    logits = jnp.dot(hidden, w_head, preferred_element_type=jnp.float32)
    scaled = logits * inv_temp[:, None]
    row_max = jnp.max(scaled, axis=1, keepdims=True)
    exp_vals = jnp.exp(scaled - row_max)
    probabilities = exp_vals / jnp.sum(exp_vals, axis=1, keepdims=True)
    cdf_table = jnp.cumsum(probabilities, axis=1)
    cdf_at_target = jnp.take_along_axis(cdf_table, target_ids[:, None], axis=1)[:, 0]
    return cdf_table, cdf_at_target
```

```python
import functools
import math

import jax
import jax.numpy as jnp
from jax import lax
from jax.experimental import pallas as pl
from jax.experimental.pallas import tpu as pltpu
from jax.sharding import PartitionSpec as P

MESH = pl.DeviceIdType.MESH
SUB = 4
LANES = 128
TILE = 256
SLOTS = 4
LOW = -3.0e38


def torus_offsets(side):
    near = sorted(
        ((dy, dx) for dy in range(side) for dx in range(side)),
        key=lambda o: (min(o[0], side - o[0]) + min(o[1], side - o[1])),
    )
    return near[1:] + near[:1]


def kernel(n, hid_hbm, w_hbm, inv_ref, tgt_ref, out_ref, pick_ref, hid, wbuf, send, recv, invcol, tcol, tri, stat,
           stat_out, stat_in, scale, offset, tval, tall, hsem, wsem, ssem, rsem, stat_ss, stat_rs, t_ss, t_rs):
    me = lax.axis_index("vp")
    rows, depth = hid.shape
    local_vocab = w_hbm.shape[1]
    tiles = local_vocab // TILE
    own_groups = rows // n // SUB
    width = 2 * tiles + 8
    side = math.isqrt(n // 2)
    core, x, y = me % 2, (me // 2) % side, me // (2 * side)

    def w_copy(t):
        return pltpu.make_async_copy(w_hbm.at[:, pl.ds(pl.multiple_of(t * TILE, TILE), TILE)], wbuf.at[t % SLOTS], wsem.at[t % SLOTS])

    hid_copy = pltpu.make_async_copy(hid_hbm, hid, hsem)
    hid_copy.start()
    for t in range(SLOTS - 1):
        w_copy(t).start()

    barrier = pltpu.get_barrier_semaphore()

    def knock(d, c):
        pl.semaphore_signal(barrier, inc=1, device_id={"vp": lax.rem(me + d, n)}, device_id_type=MESH)
        return c

    lax.fori_loop(1, n, knock, 0)

    eye = lax.broadcasted_iota(jnp.int32, (LANES, LANES), 0) == lax.broadcasted_iota(jnp.int32, (LANES, LANES), 1)
    shard_start = (me * local_vocab).astype(jnp.float32)
    for q in range(rows // LANES):
        cut = slice(q * LANES, (q + 1) * LANES)
        for src, dst, base in ((inv_ref, invcol, 0.0), (tgt_ref, tcol, shard_start)):
            seg = jnp.broadcast_to(src[:, cut].astype(jnp.float32), (LANES, LANES))
            col = jnp.sum(jnp.where(eye, seg, 0.0), axis=1, keepdims=True) - base
            dst[cut, :] = jnp.broadcast_to(col, (LANES, LANES))
    tri[...] = (lax.broadcasted_iota(jnp.int32, (TILE, TILE), 0) <= lax.broadcasted_iota(jnp.int32, (TILE, TILE), 1)).astype(jnp.float32).astype(jnp.bfloat16)
    stat[...] = jnp.zeros_like(stat)

    def piece(ref, owner, t):
        return ref.at[pl.ds(owner * own_groups, own_groups), :, pl.ds(pl.multiple_of(t * TILE, TILE), TILE)]

    def peers():
        for dy, dx in torus_offsets(side):
            for dc in range(2):
                if (dy, dx, dc) != (0, 0, 0):
                    yield (((y + dy) % side) * side + (x + dx) % side) * 2 + (core + dc) % 2

    def send_tile(t):
        for peer in peers():
            pltpu.make_async_remote_copy(
                src_ref=piece(send, peer, t),
                dst_ref=piece(recv, me, t),
                send_sem=ssem,
                recv_sem=rsem.at[t],
                device_id={"vp": peer},
                device_id_type=MESH,
            ).start()

    def compute_tile(t):
        w_copy(t).wait()
        z = jnp.dot(hid[...], wbuf[t % SLOTS], preferred_element_type=jnp.float32)
        z = z * jnp.concatenate([invcol[...]] * (TILE // LANES), axis=1)
        top = jnp.max(z, axis=1, keepdims=True)
        e = jnp.exp(z - top)
        hi = e.astype(jnp.bfloat16)
        rest = e - hi.astype(jnp.float32)
        mid = rest.astype(jnp.bfloat16)
        low = (rest - mid.astype(jnp.float32)).astype(jnp.bfloat16)
        upto = tri[...]
        run = jnp.dot(low, upto, preferred_element_type=jnp.float32)
        run = run + jnp.dot(mid, upto, preferred_element_type=jnp.float32)
        run = run + jnp.dot(hi, upto, preferred_element_type=jnp.float32)
        at = lax.broadcasted_iota(jnp.int32, (rows, TILE), 1).astype(jnp.float32) + (t * TILE).astype(jnp.float32)
        tc = jnp.concatenate([tcol[...]] * (TILE // LANES), axis=1)
        hit = jnp.sum(jnp.where(at == tc, run, 0.0), axis=1, keepdims=True)
        lane = lax.broadcasted_iota(jnp.int32, (rows, LANES), 1)
        st = stat[...]
        st = jnp.where(lane == t, top, st)
        st = jnp.where(lane == tiles + t, run[:, TILE - 1 :], st)
        st = jnp.where(lane == 2 * tiles, st + hit, st)
        stat[...] = st
        cols = pl.ds(pl.multiple_of(t * TILE, TILE), TILE)
        for k in range(rows // SUB):
            send[k, :, cols] = run[k * SUB : (k + 1) * SUB]
        own = pl.ds(me * own_groups, own_groups)
        recv[own, :, cols] = send[own, :, cols]

    hid_copy.wait()

    def step(t, c):
        @pl.when(t + SLOTS - 1 < tiles)
        def _():
            w_copy(t + SLOTS - 1).start()

        compute_tile(t)

        @pl.when(t == 0)
        def _():
            pl.semaphore_wait(barrier, n - 1)

        @pl.when(t % 2 == 0)
        def _():
            send_tile(t // 2)

        return c

    lax.fori_loop(0, tiles, step, 0)

    lane8 = lax.broadcasted_iota(jnp.int32, (rows, LANES), 1)
    stat[...] = jnp.where(lane8 == 2 * tiles + 1, tcol[...], stat[...])
    for i in range(n):
        block = None
        for g in range(own_groups):
            k = i * own_groups + g
            part = stat[k * SUB : (k + 1) * SUB, :]
            part = part if g == 0 else pltpu.roll(part, g * width, 1)
            block = part if block is None else block + part
        stat_out[i] = block
    stat_in[me] = stat_out[me]
    for peer in peers():
        pltpu.make_async_remote_copy(
            src_ref=stat_out.at[peer], dst_ref=stat_in.at[me], send_sem=stat_ss, recv_sem=stat_rs,
            device_id={"vp": peer}, device_id_type=MESH,
        ).start()

    half = tiles // 2
    more = half + tiles // 4

    def send_more(t, c):
        send_tile(t)
        return c

    lax.fori_loop(half, more, send_more, 0)

    pltpu.make_async_copy(stat_in.at[pl.ds(0, n - 1)], stat_in.at[pl.ds(0, n - 1)], stat_rs).wait()

    lane = lax.broadcasted_iota(jnp.int32, (n, SUB, LANES), 2)
    first = lane < tiles
    values = []
    for g in range(own_groups):
        got = stat_in[...]
        if g:
            got = pltpu.roll(got, LANES - g * width, 2)
        tops = jnp.where(first, got, LOW)
        top = jnp.max(jnp.max(tops, axis=0, keepdims=True), axis=2, keepdims=True)
        weight = jnp.where(first, jnp.exp(tops - top), 0.0)
        mass = weight * jnp.where(first, pltpu.roll(got, LANES - tiles, 2), 0.0)
        upto = mass
        shift = 1
        while shift < tiles:
            upto = upto + jnp.where(lane >= shift, pltpu.roll(upto, shift, 2), 0.0)
            shift *= 2
        before = jnp.where(lane >= 1, pltpu.roll(upto, 1, 2), 0.0)
        shard = jnp.sum(mass, axis=2, keepdims=True)
        start = jnp.zeros((1, SUB, 1), jnp.float32)
        starts = []
        for s in range(n):
            starts.append(start)
            start = start + shard[s : s + 1]
        inv = 1.0 / start
        sc = weight * inv
        of = (before + jnp.concatenate(starts, axis=0)) * inv
        scale[g] = sc
        offset[g] = of
        picked = jnp.broadcast_to(got[:, :, 2 * tiles : 2 * tiles + 1], got.shape)
        target = jnp.broadcast_to(got[:, :, 2 * tiles + 1 : 2 * tiles + 2], got.shape)
        lo = (lane * TILE).astype(jnp.float32)
        hit = first & (target >= lo) & (target < lo + float(TILE))
        val = jnp.where(hit, sc * picked + of, 0.0)
        values.append(jnp.sum(jnp.sum(val, axis=0), axis=1, keepdims=True))
    lane4 = lax.broadcasted_iota(jnp.int32, (SUB, LANES), 1)
    row4 = lax.broadcasted_iota(jnp.int32, (SUB, LANES), 0)
    line = jnp.zeros((SUB, LANES), jnp.float32)
    for g in range(own_groups):
        line = jnp.where(lane4 == row4 + g * SUB, values[g], line)
    line = jnp.sum(line, axis=0, keepdims=True)
    tval[...] = line
    tall[me] = line
    for peer in peers():
        pltpu.make_async_remote_copy(
            src_ref=tval, dst_ref=tall.at[me], send_sem=t_ss, recv_sem=t_rs,
            device_id={"vp": peer}, device_id_type=MESH,
        ).start()

    lax.fori_loop(more, tiles, send_more, 0)

    for t in range(tiles):
        part = recv.at[pl.ds(0, (n - 1) * own_groups), :, pl.ds(t * TILE, TILE)]
        pltpu.make_async_copy(part, part, rsem.at[t]).wait()

        def finish(s, c):
            cols = pl.ds(pl.multiple_of(s * local_vocab + t * TILE, TILE), TILE)
            for g in range(own_groups):
                sc = scale[g, s][:, t : t + 1]
                of = offset[g, s][:, t : t + 1]
                out_ref[g * SUB : (g + 1) * SUB, cols] = recv[s * own_groups + g, :, t * TILE : (t + 1) * TILE] * sc + of
            return c

        lax.fori_loop(0, n, finish, 0, unroll=4)

    pltpu.make_async_copy(tall.at[pl.ds(0, n - 1)], tall.at[pl.ds(0, n - 1)], t_rs).wait()
    own_rows = own_groups * SUB
    lane1 = lax.broadcasted_iota(jnp.int32, (1, LANES), 1)
    acc = [jnp.zeros((1, LANES), jnp.float32) for _ in range(rows // LANES)]
    for s in range(n):
        q, off = divmod(s * own_rows, LANES)
        line = tall[s]
        line = pltpu.roll(line, off, 1) if off else line
        acc[q] = acc[q] + jnp.where(lane1 >= off, line, 0.0)
        if off + own_rows > LANES:
            acc[q + 1] = acc[q + 1] + jnp.where(lane1 < off, line, 0.0)
    for q in range(rows // LANES):
        pick_ref[:, q * LANES : (q + 1) * LANES] = acc[q]

    sent = send.at[pl.ds(0, (n - 1) * own_groups)]
    pltpu.make_async_copy(sent, sent, ssem).wait()
    pltpu.make_async_copy(stat_in.at[pl.ds(0, n - 1)], stat_in.at[pl.ds(0, n - 1)], stat_ss).wait()
    pltpu.make_async_copy(tall.at[pl.ds(0, n - 1)], tall.at[pl.ds(0, n - 1)], t_ss).wait()


def solution(mesh):
    n = mesh.shape["vp"]

    def local_step(hidden, w_local, inv_temp, target_ids):
        rows, depth = hidden.shape
        local_vocab = w_local.shape[1]
        tiles = local_vocab // TILE
        groups = rows // SUB
        own_rows = rows // n
        f32 = jnp.float32
        table, picked = pl.pallas_call(
            functools.partial(kernel, n),
            out_shape=(
                pltpu.VMEM((own_rows, n * local_vocab), f32),
                jax.ShapeDtypeStruct((1, rows), f32),
            ),
            in_specs=[
                pl.BlockSpec(memory_space=pltpu.HBM),
                pl.BlockSpec(memory_space=pltpu.HBM),
                pl.BlockSpec(memory_space=pltpu.VMEM),
                pl.BlockSpec(memory_space=pltpu.VMEM),
            ],
            out_specs=(pl.BlockSpec(memory_space=pltpu.VMEM), pl.BlockSpec(memory_space=pltpu.VMEM)),
            scratch_shapes=[
                pltpu.VMEM((rows, depth), jnp.bfloat16),
                pltpu.VMEM((SLOTS, depth, TILE), jnp.bfloat16),
                pltpu.VMEM((groups, SUB, local_vocab), f32),
                pltpu.VMEM((groups, SUB, local_vocab), f32),
                pltpu.VMEM((rows, LANES), f32),
                pltpu.VMEM((rows, LANES), f32),
                pltpu.VMEM((TILE, TILE), jnp.bfloat16),
                pltpu.VMEM((rows, LANES), f32),
                pltpu.VMEM((n, SUB, LANES), f32),
                pltpu.VMEM((n, SUB, LANES), f32),
                pltpu.VMEM((own_rows // SUB, n, SUB, LANES), f32),
                pltpu.VMEM((own_rows // SUB, n, SUB, LANES), f32),
                pltpu.VMEM((1, LANES), f32),
                pltpu.VMEM((n, 1, LANES), f32),
                pltpu.SemaphoreType.DMA,
                pltpu.SemaphoreType.DMA((SLOTS,)),
                pltpu.SemaphoreType.DMA,
                pltpu.SemaphoreType.DMA((tiles,)),
                pltpu.SemaphoreType.DMA,
                pltpu.SemaphoreType.DMA,
                pltpu.SemaphoreType.DMA,
                pltpu.SemaphoreType.DMA,
            ],
            compiler_params=pltpu.CompilerParams(collective_id=0, has_side_effects=True, vmem_limit_bytes=54 << 20),
            name="head_cdf",
        )(hidden, w_local, inv_temp.reshape(1, rows), target_ids.reshape(1, rows))
        return table, picked.reshape(rows)

    return jax.shard_map(
        local_step,
        mesh=mesh,
        in_specs=(P("dp", None), P(None, "vp"), P("dp"), P("dp")),
        out_specs=(P(("dp", "vp"), None), P("dp")),
        check_vma=False,
    )
```

```python
import functools
import math

import jax
import jax.numpy as jnp
from jax import lax
from jax.experimental import pallas as pl
from jax.experimental.pallas import tpu as pltpu
from jax.sharding import PartitionSpec as P

MESH = pl.DeviceIdType.MESH
SUB = 4
LANES = 128
TILE = 256
PIECE = 128
SLOTS = 4
PARTS = 4
WINDOW = 5
LAG = 4
LOW = -3.0e38


def torus_offsets(side):
    def hops(d):
        return min(d, side - d)

    near = sorted(
        ((dy, dx) for dy in range(side) for dx in range(side)),
        key=lambda o: (hops(o[0]) + hops(o[1]), abs(hops(o[0]) - hops(o[1]))),
    )
    return near[1:] + near[:1]


def kernel(n, hid_hbm, w_hbm, inv_ref, tgt_ref, out_ref, pick_ref, hid, wbuf, send, recv, invcol, tcol, tri, stat,
           stat_out, stat_in, scale, offset, scale_b, offset_b, tval, tall, hsem, wsem, ssem, rsem, stat_ss, stat_rs,
           t_ss, t_rs):
    me = lax.axis_index("vp")
    rows, depth = hid.shape
    local_vocab = w_hbm.shape[1]
    tiles = local_vocab // TILE
    rounds = local_vocab // PIECE
    per = TILE // PIECE
    own_groups = rows // n // SUB
    width = 2 * tiles + 8
    side = math.isqrt(n // 2)
    core, x, y = me % 2, (me // 2) % side, me // (2 * side)
    settle = tiles + LAG

    def w_start(t):
        cols = pl.ds(pl.multiple_of(t * TILE, TILE), TILE)
        for p in range(PARTS):
            part = pl.ds(p * (depth // PARTS), depth // PARTS)
            pltpu.make_async_copy(w_hbm.at[part, cols], wbuf.at[t % SLOTS, part], wsem.at[t % SLOTS]).start()

    for p in range(PARTS):
        part = pl.ds(p * (rows // PARTS), rows // PARTS)
        pltpu.make_async_copy(hid_hbm.at[part], hid.at[part], hsem).start()
    w_start(jnp.int32(0))

    barrier = pltpu.get_barrier_semaphore()

    def knock(d, c):
        pl.semaphore_signal(barrier, inc=1, device_id={"vp": lax.rem(me + d, n)}, device_id_type=MESH)
        return c

    lax.fori_loop(1, n, knock, 0)

    eye = lax.broadcasted_iota(jnp.int32, (LANES, LANES), 0) == lax.broadcasted_iota(jnp.int32, (LANES, LANES), 1)
    shard_start = (me * local_vocab).astype(jnp.float32)
    for q in range(rows // LANES):
        cut = slice(q * LANES, (q + 1) * LANES)
        for src, dst, base in ((inv_ref, invcol, 0.0), (tgt_ref, tcol, shard_start)):
            seg = jnp.broadcast_to(src[cut].reshape(1, LANES).astype(jnp.float32), (LANES, LANES))
            col = jnp.sum(jnp.where(eye, seg, 0.0), axis=1, keepdims=True) - base
            dst[cut, :] = jnp.broadcast_to(col, (LANES, LANES))
    tri[...] = (lax.broadcasted_iota(jnp.int32, (TILE, TILE), 0) <= lax.broadcasted_iota(jnp.int32, (TILE, TILE), 1)).astype(jnp.float32).astype(jnp.bfloat16)
    stat[...] = jnp.zeros_like(stat)

    def piece(ref, owner, r):
        return ref.at[pl.ds(owner * own_groups, own_groups), :, pl.ds(pl.multiple_of(r * PIECE, PIECE), PIECE)]

    def peers():
        for dy, dx in torus_offsets(side):
            for dc in range(2):
                if (dy, dx, dc) != (0, 0, 0):
                    yield (((y + dy) % side) * side + (x + dx) % side) * 2 + (core + dc) % 2

    def send_round(r):
        for peer in peers():
            pltpu.make_async_remote_copy(
                src_ref=piece(send, peer, r),
                dst_ref=piece(recv, me, r),
                send_sem=ssem.at[r],
                recv_sem=rsem.at[r],
                device_id={"vp": peer},
                device_id_type=MESH,
            ).start()

    def sent_round(r):
        part = send.at[pl.ds(0, (n - 1) * own_groups), :, pl.ds(0, PIECE)]
        pltpu.make_async_copy(part, part, ssem.at[r]).wait()

    def compute_tile(t):
        pltpu.make_async_copy(wbuf.at[t % SLOTS], wbuf.at[t % SLOTS], wsem.at[t % SLOTS]).wait()

        @pl.when(t == 0)
        def _():
            w_start(t + 1)

        @pl.when(t + 2 < tiles)
        def _():
            w_start(t + 2)

        z = jnp.dot(hid[...], wbuf[t % SLOTS], preferred_element_type=jnp.float32)
        z = z * jnp.concatenate([invcol[...]] * (TILE // LANES), axis=1)
        top = jnp.max(z, axis=1, keepdims=True)
        e = jnp.exp(z - top)
        hi = e.astype(jnp.bfloat16)
        rest = e - hi.astype(jnp.float32)
        mid = rest.astype(jnp.bfloat16)
        low = (rest - mid.astype(jnp.float32)).astype(jnp.bfloat16)
        upto = tri[...]
        run = jnp.dot(low, upto, preferred_element_type=jnp.float32)
        run = run + jnp.dot(mid, upto, preferred_element_type=jnp.float32)
        run = run + jnp.dot(hi, upto, preferred_element_type=jnp.float32)
        cols = pl.ds(pl.multiple_of(t * TILE, TILE), TILE)
        for k in range(rows // SUB):
            send[k, :, cols] = run[k * SUB : (k + 1) * SUB]
        at = lax.broadcasted_iota(jnp.int32, (rows, TILE), 1).astype(jnp.float32) + (t * TILE).astype(jnp.float32)
        tc = jnp.concatenate([tcol[...]] * (TILE // LANES), axis=1)
        hit = jnp.sum(jnp.where(at == tc, run, 0.0), axis=1, keepdims=True)
        lane = lax.broadcasted_iota(jnp.int32, (rows, LANES), 1)
        st = stat[...]
        st = jnp.where(lane == t, top, st)
        st = jnp.where(lane == tiles + t, run[:, TILE - 1 :], st)
        st = jnp.where(lane == 2 * tiles, st + hit, st)
        stat[...] = st
        own = pl.ds(me * own_groups, own_groups)
        recv[own, :, cols] = send[own, :, cols]

    def send_statistics():
        lane8 = lax.broadcasted_iota(jnp.int32, (rows, LANES), 1)
        stat[...] = jnp.where(lane8 == 2 * tiles + 1, tcol[...], stat[...])
        for i in range(n):
            block = None
            for g in range(own_groups):
                k = i * own_groups + g
                part = stat[k * SUB : (k + 1) * SUB, :]
                part = part if g == 0 else pltpu.roll(part, g * width, 1)
                block = part if block is None else block + part
            stat_out[i] = block
        stat_in[me] = stat_out[me]

        def go(d, c):
            peer = lax.rem(me + d, n)
            pltpu.make_async_remote_copy(
                src_ref=stat_out.at[peer], dst_ref=stat_in.at[me], send_sem=stat_ss, recv_sem=stat_rs,
                device_id={"vp": peer}, device_id_type=MESH,
            ).start()
            return c

        lax.fori_loop(1, n, go, 0)

    def take_statistics():
        pltpu.make_async_copy(stat_in.at[pl.ds(0, n - 1)], stat_in.at[pl.ds(0, n - 1)], stat_rs).wait()
        lane = lax.broadcasted_iota(jnp.int32, (n, SUB, LANES), 2)
        first = lane < tiles
        lane4 = lax.broadcasted_iota(jnp.int32, (SUB, LANES), 1)
        row4 = lax.broadcasted_iota(jnp.int32, (SUB, LANES), 0)
        line = jnp.zeros((SUB, LANES), jnp.float32)
        for g in range(own_groups):
            got = stat_in[...]
            if g:
                got = pltpu.roll(got, LANES - g * width, 2)
            tops = jnp.where(first, got, LOW)
            top = jnp.max(jnp.max(tops, axis=0, keepdims=True), axis=2, keepdims=True)
            weight = jnp.where(first, jnp.exp(tops - top), 0.0)
            mass = weight * jnp.where(first, pltpu.roll(got, LANES - tiles, 2), 0.0)
            upto = mass
            shift = 1
            while shift < tiles:
                upto = upto + jnp.where(lane >= shift, pltpu.roll(upto, shift, 2), 0.0)
                shift *= 2
            before = jnp.where(lane >= 1, pltpu.roll(upto, 1, 2), 0.0)
            shard = jnp.sum(mass, axis=2, keepdims=True)
            start = jnp.zeros((1, SUB, 1), jnp.float32)
            starts = []
            for s in range(n):
                starts.append(start)
                start = start + shard[s : s + 1]
            inv = 1.0 / start
            sc = weight * inv
            of = (before + jnp.concatenate(starts, axis=0)) * inv
            scale[g] = sc
            offset[g] = of
            picked = jnp.broadcast_to(got[:, :, 2 * tiles : 2 * tiles + 1], got.shape)
            target = jnp.broadcast_to(got[:, :, 2 * tiles + 1 : 2 * tiles + 2], got.shape)
            lo = (lane * TILE).astype(jnp.float32)
            hit = first & (target >= lo) & (target < lo + float(TILE))
            val = jnp.where(hit, sc * picked + of, 0.0)
            val = jnp.sum(jnp.sum(val, axis=0), axis=1, keepdims=True)
            line = jnp.where(lane4 == row4 + g * SUB, val, line)
        line = jnp.sum(line, axis=0, keepdims=True)
        tval[...] = line
        tall[me] = line

        def go(d, c):
            pltpu.make_async_remote_copy(
                src_ref=tval, dst_ref=tall.at[me], send_sem=t_ss, recv_sem=t_rs,
                device_id={"vp": lax.rem(me + d, n)}, device_id_type=MESH,
            ).start()
            return c

        lax.fori_loop(1, n, go, 0)

        def spread(t, c):
            for g in range(own_groups):
                for ref, wide in ((scale, scale_b), (offset, offset_b)):
                    v = ref[g]
                    wide[t, g] = jnp.broadcast_to(v[:, :, :1], v.shape)
                    ref[g] = pltpu.roll(v, LANES - 1, 2)
            return c

        lax.fori_loop(0, tiles, spread, 0)

    def finish_round(r):
        part = recv.at[pl.ds(0, (n - 1) * own_groups), :, pl.ds(0, PIECE)]
        pltpu.make_async_copy(part, part, rsem.at[r]).wait()
        t = r // per
        here = pl.ds(pl.multiple_of(r * PIECE, PIECE), PIECE)

        def one(s, c):
            cols = pl.ds(pl.multiple_of(s * local_vocab + r * PIECE, PIECE), PIECE)
            for g in range(own_groups):
                out_ref[g * SUB : (g + 1) * SUB, cols] = recv[s * own_groups + g, :, here] * scale_b[t, g, s] + offset_b[t, g, s]
            return c

        lax.fori_loop(0, n, one, 0, unroll=8)

    pltpu.make_async_copy(hid, hid, hsem).wait()

    def step(r, c):
        @pl.when(r < tiles)
        def _():
            compute_tile(r)

        @pl.when(r == 0)
        def _():
            pl.semaphore_wait(barrier, n - 1)

        @pl.when(r == tiles)
        def _():
            send_statistics()

        @pl.when(r == settle)
        def _():
            take_statistics()

        @pl.when(r >= WINDOW)
        def _():
            sent_round(r - WINDOW)

        send_round(r)

        @pl.when(r >= settle)
        def _():
            finish_round((r - settle) * 2)
            finish_round((r - settle) * 2 + 1)

        return c

    lax.fori_loop(0, rounds, step, 0)

    pltpu.make_async_copy(tall.at[pl.ds(0, n - 1)], tall.at[pl.ds(0, n - 1)], t_rs).wait()
    own_rows = own_groups * SUB
    lane1 = lax.broadcasted_iota(jnp.int32, (1, LANES), 1)
    acc = [jnp.zeros((1, LANES), jnp.float32) for _ in range(rows // LANES)]
    for s in range(n):
        q, off = divmod(s * own_rows, LANES)
        line = tall[s]
        line = pltpu.roll(line, off, 1) if off else line
        acc[q] = acc[q] + jnp.where(lane1 >= off, line, 0.0)
        if off + own_rows > LANES:
            acc[q + 1] = acc[q + 1] + jnp.where(lane1 < off, line, 0.0)
    for q in range(rows // LANES):
        pick_ref[q * LANES : (q + 1) * LANES] = acc[q].reshape(LANES)

    def last(r, c):
        finish_round(r)
        return c

    lax.fori_loop((rounds - settle) * 2, rounds, last, 0)

    def left(r, c):
        sent_round(r)
        return c

    lax.fori_loop(rounds - WINDOW, rounds, left, 0)
    pltpu.make_async_copy(stat_in.at[pl.ds(0, n - 1)], stat_in.at[pl.ds(0, n - 1)], stat_ss).wait()
    pltpu.make_async_copy(tall.at[pl.ds(0, n - 1)], tall.at[pl.ds(0, n - 1)], t_ss).wait()


def solution(mesh):
    n = mesh.shape["vp"]

    def local_step(hidden, w_local, inv_temp, target_ids):
        rows, depth = hidden.shape
        local_vocab = w_local.shape[1]
        tiles = local_vocab // TILE
        groups = rows // SUB
        own_rows = rows // n
        f32 = jnp.float32
        table, picked = pl.pallas_call(
            functools.partial(kernel, n),
            out_shape=(
                pltpu.VMEM((own_rows, n * local_vocab), f32),
                jax.ShapeDtypeStruct((rows,), f32),
            ),
            in_specs=[
                pl.BlockSpec(memory_space=pltpu.HBM),
                pl.BlockSpec(memory_space=pltpu.HBM),
                pl.BlockSpec(memory_space=pltpu.VMEM),
                pl.BlockSpec(memory_space=pltpu.VMEM),
            ],
            out_specs=(pl.BlockSpec(memory_space=pltpu.VMEM), pl.BlockSpec(memory_space=pltpu.VMEM)),
            scratch_shapes=[
                pltpu.VMEM((rows, depth), jnp.bfloat16),
                pltpu.VMEM((SLOTS, depth, TILE), jnp.bfloat16),
                pltpu.VMEM((groups, SUB, local_vocab), f32),
                pltpu.VMEM((groups, SUB, local_vocab), f32),
                pltpu.VMEM((rows, LANES), f32),
                pltpu.VMEM((rows, LANES), f32),
                pltpu.VMEM((TILE, TILE), jnp.bfloat16),
                pltpu.VMEM((rows, LANES), f32),
                pltpu.VMEM((n, SUB, LANES), f32),
                pltpu.VMEM((n, SUB, LANES), f32),
                pltpu.VMEM((own_rows // SUB, n, SUB, LANES), f32),
                pltpu.VMEM((own_rows // SUB, n, SUB, LANES), f32),
                pltpu.VMEM((tiles, own_rows // SUB, n, SUB, LANES), f32),
                pltpu.VMEM((tiles, own_rows // SUB, n, SUB, LANES), f32),
                pltpu.VMEM((1, LANES), f32),
                pltpu.VMEM((n, 1, LANES), f32),
                pltpu.SemaphoreType.DMA,
                pltpu.SemaphoreType.DMA((SLOTS,)),
                pltpu.SemaphoreType.DMA((local_vocab // PIECE,)),
                pltpu.SemaphoreType.DMA((local_vocab // PIECE,)),
                pltpu.SemaphoreType.DMA,
                pltpu.SemaphoreType.DMA,
                pltpu.SemaphoreType.DMA,
                pltpu.SemaphoreType.DMA,
            ],
            compiler_params=pltpu.CompilerParams(collective_id=0, has_side_effects=True, vmem_limit_bytes=54 << 20),
            name="head_cdf",
        )(hidden, w_local, inv_temp, target_ids)
        return table, picked

    return jax.shard_map(
        local_step,
        mesh=mesh,
        in_specs=(P("dp", None), P(None, "vp"), P("dp"), P("dp")),
        out_specs=(P(("dp", "vp"), None), P("dp")),
        check_vma=False,
    )
```

```python
import functools
import math

import jax
import jax.numpy as jnp
from jax import lax
from jax.experimental import pallas as pl
from jax.experimental.pallas import tpu as pltpu
from jax.sharding import PartitionSpec as P

MESH = pl.DeviceIdType.MESH
SUB = 4
LANES = 128
TILE = 256
SLOTS = 3
PARTS = 4
LOW = -3.0e38


def kernel(n, hid_hbm, w_hbm, inv_ref, tgt_ref, out_ref, pick_ref, hid, wbuf, send, mid, recv, invcol, tcol, tri, stat,
           stat_out, stat_in, scale, offset, scale_b, offset_b, tval, tall, hsem, wsem, one_ss, one_rs, two_ss, two_rs,
           stat_ss, stat_rs, t_ss, t_rs):
    me = lax.axis_index("vp")
    rows, depth = hid.shape
    local_vocab = w_hbm.shape[1]
    tiles = local_vocab // TILE
    own_groups = rows // n // SUB
    width = 2 * tiles + 8
    side = math.isqrt(n // 2)
    core, x, y = me % 2, (me // 2) % side, me // (2 * side)
    a = x + core * (y - x)
    b = y + core * (x - y)

    def device(a_, b_, core_):
        row = b_ + core * (a_ - b_)
        col = a_ + core * (b_ - a_)
        return {"vp": (row * side + col) * 2 + core_}

    slab = 2 * side * own_groups

    def w_start(t):
        cols = pl.ds(pl.multiple_of(t * TILE, TILE), TILE)
        for p in range(PARTS):
            part = pl.ds(p * (depth // PARTS), depth // PARTS)
            pltpu.make_async_copy(w_hbm.at[part, cols], wbuf.at[t % SLOTS, part], wsem.at[t % SLOTS]).start()

    for p in range(PARTS):
        part = pl.ds(p * (rows // PARTS), rows // PARTS)
        pltpu.make_async_copy(hid_hbm.at[part], hid.at[part], hsem).start()
    w_start(jnp.int32(0))

    barrier = pltpu.get_barrier_semaphore()

    def knock(d, c):
        pl.semaphore_signal(barrier, inc=1, device_id={"vp": lax.rem(me + d, n)}, device_id_type=MESH)
        return c

    lax.fori_loop(1, n, knock, 0)

    eye = lax.broadcasted_iota(jnp.int32, (LANES, LANES), 0) == lax.broadcasted_iota(jnp.int32, (LANES, LANES), 1)
    shard_start = (me * local_vocab).astype(jnp.float32)
    for q in range(rows // LANES):
        cut = slice(q * LANES, (q + 1) * LANES)
        for src, dst, base in ((inv_ref, invcol, 0.0), (tgt_ref, tcol, shard_start)):
            seg = jnp.broadcast_to(src[cut].reshape(1, LANES).astype(jnp.float32), (LANES, LANES))
            col = jnp.sum(jnp.where(eye, seg, 0.0), axis=1, keepdims=True) - base
            dst[cut, :] = jnp.broadcast_to(col, (LANES, LANES))
    tri[...] = (lax.broadcasted_iota(jnp.int32, (TILE, TILE), 0) <= lax.broadcasted_iota(jnp.int32, (TILE, TILE), 1)).astype(jnp.float32).astype(jnp.bfloat16)
    stat[...] = jnp.zeros_like(stat)

    def columns(t):
        return pl.ds(pl.multiple_of(t * TILE, TILE), TILE)

    def first_leg(r):
        for hop in (1, side - 1, *range(2, side - 1)):
            to = (a + hop) % side
            pltpu.make_async_remote_copy(
                src_ref=send.at[pl.ds(to * slab, slab), :, columns(r)],
                dst_ref=mid.at[a, :, :, columns(r)],
                send_sem=one_ss,
                recv_sem=one_rs.at[r],
                device_id=device(to, b, core),
                device_id_type=MESH,
            ).start()

    def second_leg(r):
        part = mid.at[pl.ds(0, side - 1), :, :, pl.ds(0, TILE)]
        pltpu.make_async_copy(part, part, one_rs.at[r]).wait()

        def onward(to, core_):
            pltpu.make_async_remote_copy(
                src_ref=mid.at[:, pl.ds((to * 2 + core_) * own_groups, own_groups), :, columns(r)],
                dst_ref=recv.at[core * side + b, :, :, :, columns(r)],
                send_sem=two_ss,
                recv_sem=two_rs.at[r],
                device_id=device(a, to, core_),
                device_id_type=MESH,
            ).start()

        for hop in (1, side - 1, *range(2, side - 1)):
            for core_ in range(2):
                onward((b + hop) % side, core_)
        onward(b, 1 - core)
        recv[core * side + b, :, :, :, columns(r)] = mid[:, pl.ds((b * 2 + core) * own_groups, own_groups), :, columns(r)]

    def compute_tile(t):
        pltpu.make_async_copy(wbuf.at[t % SLOTS], wbuf.at[t % SLOTS], wsem.at[t % SLOTS]).wait()

        @pl.when(t == 0)
        def _():
            w_start(t + 1)

        @pl.when(t + 2 < tiles)
        def _():
            w_start(t + 2)

        z = jnp.dot(hid[...], wbuf[t % SLOTS], preferred_element_type=jnp.float32)
        z = z * jnp.concatenate([invcol[...]] * (TILE // LANES), axis=1)
        top = jnp.max(z, axis=1, keepdims=True)
        e = jnp.exp(z - top)
        hi = e.astype(jnp.bfloat16)
        rest = e - hi.astype(jnp.float32)
        more = rest.astype(jnp.bfloat16)
        low = (rest - more.astype(jnp.float32)).astype(jnp.bfloat16)
        upto = tri[...]
        run = jnp.dot(low, upto, preferred_element_type=jnp.float32)
        run = run + jnp.dot(more, upto, preferred_element_type=jnp.float32)
        run = run + jnp.dot(hi, upto, preferred_element_type=jnp.float32)
        cols = columns(t)
        for k in range(rows // SUB):
            owner, g = divmod(k, own_groups)
            oy, ox, oc = owner // (2 * side), (owner // 2) % side, owner % 2
            x_first, y_first = ((ox * side + oy) * 2 + oc) * own_groups + g, ((oy * side + ox) * 2 + oc) * own_groups + g
            send[x_first + core * (y_first - x_first), :, cols] = run[k * SUB : (k + 1) * SUB]
        at = lax.broadcasted_iota(jnp.int32, (rows, TILE), 1).astype(jnp.float32) + (t * TILE).astype(jnp.float32)
        tc = jnp.concatenate([tcol[...]] * (TILE // LANES), axis=1)
        hit = jnp.sum(jnp.where(at == tc, run, 0.0), axis=1, keepdims=True)
        lane = lax.broadcasted_iota(jnp.int32, (rows, LANES), 1)
        st = stat[...]
        st = jnp.where(lane == t, top, st)
        st = jnp.where(lane == tiles + t, run[:, TILE - 1 :], st)
        st = jnp.where(lane == 2 * tiles, st + hit, st)
        stat[...] = st
        mid[a, :, :, cols] = send[pl.ds(a * slab, slab), :, cols]

    def send_statistics():
        lane8 = lax.broadcasted_iota(jnp.int32, (rows, LANES), 1)
        stat[...] = jnp.where(lane8 == 2 * tiles + 1, tcol[...], stat[...])
        for i in range(n):
            block = None
            for g in range(own_groups):
                k = i * own_groups + g
                part = stat[k * SUB : (k + 1) * SUB, :]
                part = part if g == 0 else pltpu.roll(part, g * width, 1)
                block = part if block is None else block + part
            stat_out[i] = block
        stat_in[me] = stat_out[me]

        def go(d, c):
            peer = lax.rem(me + d, n)
            pltpu.make_async_remote_copy(
                src_ref=stat_out.at[peer], dst_ref=stat_in.at[me], send_sem=stat_ss, recv_sem=stat_rs,
                device_id={"vp": peer}, device_id_type=MESH,
            ).start()
            return c

        lax.fori_loop(1, n, go, 0)

    def take_statistics():
        pltpu.make_async_copy(stat_in.at[pl.ds(0, n - 1)], stat_in.at[pl.ds(0, n - 1)], stat_rs).wait()
        lane = lax.broadcasted_iota(jnp.int32, (n, SUB, LANES), 2)
        first = lane < tiles
        lane4 = lax.broadcasted_iota(jnp.int32, (SUB, LANES), 1)
        row4 = lax.broadcasted_iota(jnp.int32, (SUB, LANES), 0)
        line = jnp.zeros((SUB, LANES), jnp.float32)
        for g in range(own_groups):
            got = stat_in[...]
            if g:
                got = pltpu.roll(got, LANES - g * width, 2)
            tops = jnp.where(first, got, LOW)
            top = jnp.max(jnp.max(tops, axis=0, keepdims=True), axis=2, keepdims=True)
            weight = jnp.where(first, jnp.exp(tops - top), 0.0)
            mass = weight * jnp.where(first, pltpu.roll(got, LANES - tiles, 2), 0.0)
            upto = mass
            shift = 1
            while shift < tiles:
                upto = upto + jnp.where(lane >= shift, pltpu.roll(upto, shift, 2), 0.0)
                shift *= 2
            before = jnp.where(lane >= 1, pltpu.roll(upto, 1, 2), 0.0)
            shard = jnp.sum(mass, axis=2, keepdims=True)
            start = jnp.zeros((1, SUB, 1), jnp.float32)
            starts = []
            for s in range(n):
                starts.append(start)
                start = start + shard[s : s + 1]
            inv = 1.0 / start
            sc = weight * inv
            of = (before + jnp.concatenate(starts, axis=0)) * inv
            scale[g] = sc
            offset[g] = of
            picked = jnp.broadcast_to(got[:, :, 2 * tiles : 2 * tiles + 1], got.shape)
            target = jnp.broadcast_to(got[:, :, 2 * tiles + 1 : 2 * tiles + 2], got.shape)
            lo = (lane * TILE).astype(jnp.float32)
            hit = first & (target >= lo) & (target < lo + float(TILE))
            val = jnp.where(hit, sc * picked + of, 0.0)
            val = jnp.sum(jnp.sum(val, axis=0), axis=1, keepdims=True)
            line = jnp.where(lane4 == row4 + g * SUB, val, line)
        line = jnp.sum(line, axis=0, keepdims=True)
        tval[...] = line
        tall[me] = line

        def go(d, c):
            pltpu.make_async_remote_copy(
                src_ref=tval, dst_ref=tall.at[me], send_sem=t_ss, recv_sem=t_rs,
                device_id={"vp": lax.rem(me + d, n)}, device_id_type=MESH,
            ).start()
            return c

        lax.fori_loop(1, n, go, 0)

        def spread(t, c):
            for g in range(own_groups):
                for ref, wide in ((scale, scale_b), (offset, offset_b)):
                    v = ref[g]
                    wide[t, g] = jnp.broadcast_to(v[:, :, :1], v.shape)
                    ref[g] = pltpu.roll(v, LANES - 1, 2)
            return c

        lax.fori_loop(0, tiles, spread, 0)

    def finish_round(r):
        part = recv.at[pl.ds(0, 2 * side - 1), :, :, :, pl.ds(0, TILE)]
        pltpu.make_async_copy(part, part, two_rs.at[r]).wait()

        def one(q, c):
            relay, u = q // side, q % side
            core_, v = relay // side, relay % side
            row = v + core_ * (u - v)
            col = u + core_ * (v - u)
            s = (row * side + col) * 2 + core_
            for g in range(own_groups):
                sc, of = scale_b[r, g, s], offset_b[r, g, s]
                for h in range(TILE // LANES):
                    here = pl.ds(pl.multiple_of(r * TILE + h * LANES, LANES), LANES)
                    cols = pl.ds(pl.multiple_of(s * local_vocab + r * TILE + h * LANES, LANES), LANES)
                    out_ref[g * SUB : (g + 1) * SUB, cols] = recv[relay, u, g, :, here] * sc + of
            return c

        lax.fori_loop(0, n, one, 0, unroll=4)

    pltpu.make_async_copy(hid, hid, hsem).wait()

    def early(t, c):
        compute_tile(t)

        @pl.when(t == 0)
        def _():
            pl.semaphore_wait(barrier, n - 1)
            first_leg(t)

        @pl.when(t == 1)
        def _():
            first_leg(t)

        @pl.when((t >= 2) & (t % 2 == 0))
        def _():
            first_leg(t // 2 + 1)

        @pl.when((t >= 3) & (t % 2 == 1))
        def _():
            second_leg((t - 3) // 2)

        return c

    lax.fori_loop(0, tiles, early, 0)
    gone = tiles // 2 + 1
    send_statistics()

    take_at = gone + 3

    def late(k, c):
        first_leg(k)

        @pl.when(k == take_at)
        def _():
            take_statistics()

        second_leg(k - 2)

        @pl.when(k >= take_at)
        def _():
            for m in range(3):
                finish_round((k - take_at) * 3 + m)

        return c

    lax.fori_loop(gone, tiles, late, 0)
    done = (tiles - take_at) * 3
    second_leg(tiles - 2)
    second_leg(tiles - 1)

    pltpu.make_async_copy(tall.at[pl.ds(0, n - 1)], tall.at[pl.ds(0, n - 1)], t_rs).wait()
    own_rows = own_groups * SUB
    lane1 = lax.broadcasted_iota(jnp.int32, (1, LANES), 1)
    acc = [jnp.zeros((1, LANES), jnp.float32) for _ in range(rows // LANES)]
    for s in range(n):
        q, off = divmod(s * own_rows, LANES)
        line = tall[s]
        line = pltpu.roll(line, off, 1) if off else line
        acc[q] = acc[q] + jnp.where(lane1 >= off, line, 0.0)
        if off + own_rows > LANES:
            acc[q + 1] = acc[q + 1] + jnp.where(lane1 < off, line, 0.0)
    for q in range(rows // LANES):
        pick_ref[q * LANES : (q + 1) * LANES] = acc[q].reshape(LANES)

    def last(r, c):
        finish_round(r)
        return c

    lax.fori_loop(done, tiles, last, 0)

    pltpu.make_async_copy(mid.at[pl.ds(0, side - 1)], mid.at[pl.ds(0, side - 1)], one_ss).wait()
    pltpu.make_async_copy(recv.at[pl.ds(0, 2 * side - 1)], recv.at[pl.ds(0, 2 * side - 1)], two_ss).wait()
    pltpu.make_async_copy(stat_in.at[pl.ds(0, n - 1)], stat_in.at[pl.ds(0, n - 1)], stat_ss).wait()
    pltpu.make_async_copy(tall.at[pl.ds(0, n - 1)], tall.at[pl.ds(0, n - 1)], t_ss).wait()


def solution(mesh):
    n = mesh.shape["vp"]
    side = math.isqrt(n // 2)

    def local_step(hidden, w_local, inv_temp, target_ids):
        rows, depth = hidden.shape
        local_vocab = w_local.shape[1]
        tiles = local_vocab // TILE
        groups = rows // SUB
        own_rows = rows // n
        f32 = jnp.float32
        table, picked = pl.pallas_call(
            functools.partial(kernel, n),
            out_shape=(
                pltpu.VMEM((own_rows, n * local_vocab), f32),
                jax.ShapeDtypeStruct((rows,), f32),
            ),
            in_specs=[
                pl.BlockSpec(memory_space=pltpu.HBM),
                pl.BlockSpec(memory_space=pltpu.HBM),
                pl.BlockSpec(memory_space=pltpu.VMEM),
                pl.BlockSpec(memory_space=pltpu.VMEM),
            ],
            out_specs=(pl.BlockSpec(memory_space=pltpu.VMEM), pl.BlockSpec(memory_space=pltpu.VMEM)),
            scratch_shapes=[
                pltpu.VMEM((rows, depth), jnp.bfloat16),
                pltpu.VMEM((SLOTS, depth, TILE), jnp.bfloat16),
                pltpu.VMEM((groups, SUB, local_vocab), f32),
                pltpu.VMEM((side, groups // side, SUB, local_vocab), f32),
                pltpu.VMEM((2 * side, side, own_rows // SUB, SUB, local_vocab), f32),
                pltpu.VMEM((rows, LANES), f32),
                pltpu.VMEM((rows, LANES), f32),
                pltpu.VMEM((TILE, TILE), jnp.bfloat16),
                pltpu.VMEM((rows, LANES), f32),
                pltpu.VMEM((n, SUB, LANES), f32),
                pltpu.VMEM((n, SUB, LANES), f32),
                pltpu.VMEM((own_rows // SUB, n, SUB, LANES), f32),
                pltpu.VMEM((own_rows // SUB, n, SUB, LANES), f32),
                pltpu.VMEM((tiles, own_rows // SUB, n, SUB, LANES), f32),
                pltpu.VMEM((tiles, own_rows // SUB, n, SUB, LANES), f32),
                pltpu.VMEM((1, LANES), f32),
                pltpu.VMEM((n, 1, LANES), f32),
                pltpu.SemaphoreType.DMA,
                pltpu.SemaphoreType.DMA((SLOTS,)),
                pltpu.SemaphoreType.DMA,
                pltpu.SemaphoreType.DMA((tiles,)),
                pltpu.SemaphoreType.DMA,
                pltpu.SemaphoreType.DMA((tiles,)),
                pltpu.SemaphoreType.DMA,
                pltpu.SemaphoreType.DMA,
                pltpu.SemaphoreType.DMA,
                pltpu.SemaphoreType.DMA,
            ],
            compiler_params=pltpu.CompilerParams(collective_id=0, has_side_effects=True, vmem_limit_bytes=54 << 20),
            name="head_cdf",
        )(hidden, w_local, inv_temp, target_ids)
        return table, picked

    return jax.shard_map(
        local_step,
        mesh=mesh,
        in_specs=(P("dp", None), P(None, "vp"), P("dp"), P("dp")),
        out_specs=(P(("dp", "vp"), None), P("dp")),
        check_vma=False,
    )
```

```python
import functools
import math

import jax
import jax.numpy as jnp
from jax import lax
from jax.experimental import pallas as pl
from jax.experimental.pallas import tpu as pltpu
from jax.sharding import PartitionSpec as P

MESH = pl.DeviceIdType.MESH
SUB = 4
LANES = 128
TILE = 256
HALF = TILE // 2
SLOTS = 3
PARTS = 4
STORES = 8
LOW = -3.0e38


def kernel(n, hid_hbm, w_hbm, inv_ref, tgt_ref, out_ref, pick_ref, hid, wbuf, send, mid, recv, invcol, tcol, tri, stat,
           stat_out, stat_in, scale, offset, scale_b, offset_b, tval, tall, hsem, wsem, one_ss, one_rs, two_ss, two_rs,
           stat_ss, stat_rs, t_ss, t_rs):
    me = lax.axis_index("vp")
    rows, depth = hid.shape
    local_vocab = w_hbm.shape[1]
    tiles = local_vocab // TILE
    own_groups = rows // n // SUB
    width = 2 * tiles + 8
    side = math.isqrt(n // 2)
    core, x, y = me % 2, (me // 2) % side, me // (2 * side)
    a = x + core * (y - x)
    b = y + core * (x - y)

    def device(a_, b_, core_):
        row = b_ + core * (a_ - b_)
        col = a_ + core * (b_ - a_)
        return {"vp": (row * side + col) * 2 + core_}

    slab = 2 * side * own_groups

    def w_start(t):
        cols = pl.ds(pl.multiple_of(t * TILE, TILE), TILE)
        for p in range(PARTS):
            part = pl.ds(p * (depth // PARTS), depth // PARTS)
            pltpu.make_async_copy(w_hbm.at[part, cols], wbuf.at[t % SLOTS, part], wsem.at[t % SLOTS]).start()

    for p in range(PARTS):
        part = pl.ds(p * (rows // PARTS), rows // PARTS)
        pltpu.make_async_copy(hid_hbm.at[part], hid.at[part], hsem).start()
    w_start(jnp.int32(0))

    barrier = pltpu.get_barrier_semaphore()

    def knock(d, c):
        pl.semaphore_signal(barrier, inc=1, device_id={"vp": lax.rem(me + d, n)}, device_id_type=MESH)
        return c

    lax.fori_loop(1, n, knock, 0)

    eye = lax.broadcasted_iota(jnp.int32, (LANES, LANES), 0) == lax.broadcasted_iota(jnp.int32, (LANES, LANES), 1)
    shard_start = (me * local_vocab).astype(jnp.float32)
    for q in range(rows // LANES):
        cut = slice(q * LANES, (q + 1) * LANES)
        for src, dst, base in ((inv_ref, invcol, 0.0), (tgt_ref, tcol, shard_start)):
            seg = jnp.broadcast_to(src[cut].reshape(1, LANES).astype(jnp.float32), (LANES, LANES))
            col = jnp.sum(jnp.where(eye, seg, 0.0), axis=1, keepdims=True) - base
            dst[cut, :] = jnp.broadcast_to(col, (LANES, LANES))
    tri[...] = (lax.broadcasted_iota(jnp.int32, (TILE, TILE), 0) <= lax.broadcasted_iota(jnp.int32, (TILE, TILE), 1)).astype(jnp.float32).astype(jnp.bfloat16)
    stat[...] = jnp.zeros_like(stat)

    def columns(t):
        return pl.ds(pl.multiple_of(t * TILE, TILE), TILE)

    def round_columns(r, part):
        if part is None:
            return columns(r), r
        start = (tiles - 1) * TILE + part * HALF
        return pl.ds(start, HALF), tiles - 1 + part

    def first_leg(r, half=None):
        cols, k = round_columns(r, half)
        for hop in (1, side - 1, *range(2, side - 1)):
            to = (a + hop) % side
            pltpu.make_async_remote_copy(
                src_ref=send.at[pl.ds(to * slab, slab), :, cols],
                dst_ref=mid.at[a, :, :, cols],
                send_sem=one_ss,
                recv_sem=one_rs.at[k],
                device_id=device(to, b, core),
                device_id_type=MESH,
            ).start()

    def second_leg(r, half=None):
        cols, k = round_columns(r, half)
        part = mid.at[pl.ds(0, side - 1), :, :, pl.ds(0, TILE if half is None else HALF)]
        pltpu.make_async_copy(part, part, one_rs.at[k]).wait()

        def onward(to, core_):
            pltpu.make_async_remote_copy(
                src_ref=mid.at[:, pl.ds((to * 2 + core_) * own_groups, own_groups), :, cols],
                dst_ref=recv.at[core * side + b, :, :, :, cols],
                send_sem=two_ss,
                recv_sem=two_rs.at[k],
                device_id=device(a, to, core_),
                device_id_type=MESH,
            ).start()

        for hop in (1, side - 1, *range(2, side - 1)):
            for core_ in range(2):
                onward((b + hop) % side, core_)
        onward(b, 1 - core)
        recv[core * side + b, :, :, :, cols] = mid[:, pl.ds((b * 2 + core) * own_groups, own_groups), :, cols]

    def compute_tile(t):
        pltpu.make_async_copy(wbuf.at[t % SLOTS], wbuf.at[t % SLOTS], wsem.at[t % SLOTS]).wait()

        @pl.when(t == 0)
        def _():
            w_start(t + 1)

        @pl.when(t + 2 < tiles)
        def _():
            w_start(t + 2)

        z = jnp.dot(hid[...], wbuf[t % SLOTS], preferred_element_type=jnp.float32)
        z = z * jnp.concatenate([invcol[...]] * (TILE // LANES), axis=1)
        top = jnp.max(z, axis=1, keepdims=True)
        e = jnp.exp(z - top)
        hi = e.astype(jnp.bfloat16)
        rest = e - hi.astype(jnp.float32)
        more = rest.astype(jnp.bfloat16)
        low = (rest - more.astype(jnp.float32)).astype(jnp.bfloat16)
        upto = tri[...]
        run = jnp.dot(low, upto, preferred_element_type=jnp.float32)
        run = run + jnp.dot(more, upto, preferred_element_type=jnp.float32)
        run = run + jnp.dot(hi, upto, preferred_element_type=jnp.float32)
        cols = columns(t)
        for k in range(rows // SUB):
            owner, g = divmod(k, own_groups)
            oy, ox, oc = owner // (2 * side), (owner // 2) % side, owner % 2
            x_first, y_first = ((ox * side + oy) * 2 + oc) * own_groups + g, ((oy * side + ox) * 2 + oc) * own_groups + g
            send[x_first + core * (y_first - x_first), :, cols] = run[k * SUB : (k + 1) * SUB]
        at = lax.broadcasted_iota(jnp.int32, (rows, TILE), 1).astype(jnp.float32) + (t * TILE).astype(jnp.float32)
        tc = jnp.concatenate([tcol[...]] * (TILE // LANES), axis=1)
        hit = jnp.sum(jnp.where(at == tc, run, 0.0), axis=1, keepdims=True)
        lane = lax.broadcasted_iota(jnp.int32, (rows, LANES), 1)
        st = stat[...]
        st = jnp.where(lane == t, top, st)
        st = jnp.where(lane == tiles + t, run[:, TILE - 1 :], st)
        st = jnp.where(lane == 2 * tiles, st + hit, st)
        stat[...] = st
        mid[a, :, :, cols] = send[pl.ds(a * slab, slab), :, cols]

    def send_statistics():
        lane8 = lax.broadcasted_iota(jnp.int32, (rows, LANES), 1)
        stat[...] = jnp.where(lane8 == 2 * tiles + 1, tcol[...], stat[...])
        for i in range(n):
            block = None
            for g in range(own_groups):
                k = i * own_groups + g
                part = stat[k * SUB : (k + 1) * SUB, :]
                part = part if g == 0 else pltpu.roll(part, g * width, 1)
                block = part if block is None else block + part
            stat_out[i] = block
        stat_in[me] = stat_out[me]

        def go(d, c):
            peer = lax.rem(me + d, n)
            pltpu.make_async_remote_copy(
                src_ref=stat_out.at[peer], dst_ref=stat_in.at[me], send_sem=stat_ss, recv_sem=stat_rs,
                device_id={"vp": peer}, device_id_type=MESH,
            ).start()
            return c

        lax.fori_loop(1, n, go, 0)

    def take_statistics():
        pltpu.make_async_copy(stat_in.at[pl.ds(0, n - 1)], stat_in.at[pl.ds(0, n - 1)], stat_rs).wait()
        lane = lax.broadcasted_iota(jnp.int32, (n, SUB, LANES), 2)
        first = lane < tiles
        lane4 = lax.broadcasted_iota(jnp.int32, (SUB, LANES), 1)
        row4 = lax.broadcasted_iota(jnp.int32, (SUB, LANES), 0)
        line = jnp.zeros((SUB, LANES), jnp.float32)
        for g in range(own_groups):
            got = stat_in[...]
            if g:
                got = pltpu.roll(got, LANES - g * width, 2)
            tops = jnp.where(first, got, LOW)
            top = jnp.max(jnp.max(tops, axis=0, keepdims=True), axis=2, keepdims=True)
            weight = jnp.where(first, jnp.exp(tops - top), 0.0)
            mass = weight * jnp.where(first, pltpu.roll(got, LANES - tiles, 2), 0.0)
            upto = mass
            shift = 1
            while shift < tiles:
                upto = upto + jnp.where(lane >= shift, pltpu.roll(upto, shift, 2), 0.0)
                shift *= 2
            before = jnp.where(lane >= 1, pltpu.roll(upto, 1, 2), 0.0)
            shard = jnp.sum(mass, axis=2, keepdims=True)
            start = jnp.zeros((1, SUB, 1), jnp.float32)
            starts = []
            for s in range(n):
                starts.append(start)
                start = start + shard[s : s + 1]
            inv = 1.0 / start
            sc = weight * inv
            of = (before + jnp.concatenate(starts, axis=0)) * inv
            scale[g] = sc
            offset[g] = of
            picked = jnp.broadcast_to(got[:, :, 2 * tiles : 2 * tiles + 1], got.shape)
            target = jnp.broadcast_to(got[:, :, 2 * tiles + 1 : 2 * tiles + 2], got.shape)
            lo = (lane * TILE).astype(jnp.float32)
            hit = first & (target >= lo) & (target < lo + float(TILE))
            val = jnp.where(hit, sc * picked + of, 0.0)
            val = jnp.sum(jnp.sum(val, axis=0), axis=1, keepdims=True)
            line = jnp.where(lane4 == row4 + g * SUB, val, line)
        line = jnp.sum(line, axis=0, keepdims=True)
        tval[...] = line
        tall[me] = line

        def go(d, c):
            pltpu.make_async_remote_copy(
                src_ref=tval, dst_ref=tall.at[me], send_sem=t_ss, recv_sem=t_rs,
                device_id={"vp": lax.rem(me + d, n)}, device_id_type=MESH,
            ).start()
            return c

        lax.fori_loop(1, n, go, 0)

    def widen(t):
        for g in range(own_groups):
            for ref, wide in ((scale, scale_b), (offset, offset_b)):
                v = ref[g]
                wide[g] = jnp.broadcast_to(v[:, :, :1], v.shape)
                ref[g] = pltpu.roll(v, LANES - 1, 2)

    def finish_round(r, half=None):
        size = TILE if half is None else HALF
        base = r * TILE if half is None else (tiles - 1) * TILE + half * HALF
        if not half:
            widen(r)
        part = recv.at[pl.ds(0, 2 * side - 1), :, :, :, pl.ds(0, size)]
        pltpu.make_async_copy(part, part, two_rs.at[r if half is None else tiles - 1 + half]).wait()

        def one(q, c):
            relay, u = q // side, q % side
            core_, v = relay // side, relay % side
            row = v + core_ * (u - v)
            col = u + core_ * (v - u)
            s = (row * side + col) * 2 + core_
            for g in range(own_groups):
                sc, of = scale_b[g, s], offset_b[g, s]
                for h in range(size // LANES):
                    here = pl.ds(pl.multiple_of(base + h * LANES, LANES), LANES)
                    cols = pl.ds(pl.multiple_of(s * local_vocab + base + h * LANES, LANES), LANES)
                    out_ref[g * SUB : (g + 1) * SUB, cols] = recv[relay, u, g, :, here] * sc + of
            return c

        lax.fori_loop(0, n, one, 0, unroll=4)

    pltpu.make_async_copy(hid, hid, hsem).wait()

    def early(t, c):
        compute_tile(t)

        @pl.when(t == 0)
        def _():
            pl.semaphore_wait(barrier, n - 1)
            first_leg(t)

        @pl.when(t == 1)
        def _():
            first_leg(t)

        @pl.when((t >= 2) & (t % 2 == 0))
        def _():
            first_leg(t // 2 + 1)

        @pl.when((t >= 3) & (t % 2 == 1))
        def _():
            second_leg((t - 3) // 2)

        return c

    lax.fori_loop(0, tiles, early, 0)
    send_statistics()

    next_one, next_two = tiles // 2 + 1, tiles // 2 - 1
    first_leg(jnp.int32(next_one))
    lead = next_one + 1 - next_two
    take_at = next_two + 3

    def late(k, c):
        first_leg(k + lead)

        @pl.when(k == take_at)
        def _():
            take_statistics()

        second_leg(k)

        @pl.when(k >= take_at)
        def _():
            for m in range(3):
                finish_round((k - take_at) * 3 + m)

        return c

    stop = tiles - 1 - lead
    lax.fori_loop(next_two, stop, late, 0)
    first_leg(None, 0)
    first_leg(None, 1)

    def finish_to(lo, hi):
        def body(r, c):
            finish_round(r)
            return c

        lax.fori_loop(lo, hi, body, 0)

    def ending(k, c):
        second_leg(k)
        finish_round((k - stop) * 2 + (stop - take_at) * 3)
        finish_round((k - stop) * 2 + (stop - take_at) * 3 + 1)
        return c

    lax.fori_loop(stop, tiles - 1, ending, 0)
    second_leg(None, 0)
    second_leg(None, 1)
    finish_to((stop - take_at) * 3 + lead * 2, tiles - 1)
    pltpu.make_async_copy(tall.at[pl.ds(0, n - 1)], tall.at[pl.ds(0, n - 1)], t_rs).wait()
    own_rows = own_groups * SUB
    lane1 = lax.broadcasted_iota(jnp.int32, (1, LANES), 1)
    acc = [jnp.zeros((1, LANES), jnp.float32) for _ in range(rows // LANES)]
    for s in range(n):
        q, off = divmod(s * own_rows, LANES)
        line = tall[s]
        line = pltpu.roll(line, off, 1) if off else line
        acc[q] = acc[q] + jnp.where(lane1 >= off, line, 0.0)
        if off + own_rows > LANES:
            acc[q + 1] = acc[q + 1] + jnp.where(lane1 < off, line, 0.0)
    for q in range(rows // LANES):
        pick_ref[q * LANES : (q + 1) * LANES] = acc[q].reshape(LANES)

    finish_round(tiles - 1, 0)
    finish_round(tiles - 1, 1)

    pltpu.make_async_copy(mid.at[pl.ds(0, side - 1)], mid.at[pl.ds(0, side - 1)], one_ss).wait()
    pltpu.make_async_copy(recv.at[pl.ds(0, 2 * side - 1)], recv.at[pl.ds(0, 2 * side - 1)], two_ss).wait()
    pltpu.make_async_copy(stat_in.at[pl.ds(0, n - 1)], stat_in.at[pl.ds(0, n - 1)], stat_ss).wait()
    pltpu.make_async_copy(tall.at[pl.ds(0, n - 1)], tall.at[pl.ds(0, n - 1)], t_ss).wait()


def store_kernel(table, picked, table_out, picked_out, sem, small_sem):
    width = table.shape[1] // STORES
    copies = [pltpu.make_async_copy(picked, picked_out, small_sem)]
    for i in range(STORES):
        cols = pl.ds(i * width, width)
        copies.append(pltpu.make_async_copy(table.at[:, cols], table_out.at[:, cols], sem.at[i]))
    for copy in copies:
        copy.start()
    for copy in copies:
        copy.wait()


def solution(mesh):
    n = mesh.shape["vp"]
    side = math.isqrt(n // 2)

    def local_step(hidden, w_local, inv_temp, target_ids):
        rows, depth = hidden.shape
        local_vocab = w_local.shape[1]
        tiles = local_vocab // TILE
        groups = rows // SUB
        own_rows = rows // n
        f32 = jnp.float32
        table, picked = pl.pallas_call(
            functools.partial(kernel, n),
            out_shape=(
                pltpu.VMEM((own_rows, n * local_vocab), f32),
                pltpu.VMEM((rows,), f32),
            ),
            in_specs=[
                pl.BlockSpec(memory_space=pltpu.HBM),
                pl.BlockSpec(memory_space=pltpu.HBM),
                pl.BlockSpec(memory_space=pltpu.VMEM),
                pl.BlockSpec(memory_space=pltpu.VMEM),
            ],
            out_specs=(pl.BlockSpec(memory_space=pltpu.VMEM), pl.BlockSpec(memory_space=pltpu.VMEM)),
            scratch_shapes=[
                pltpu.VMEM((rows, depth), jnp.bfloat16),
                pltpu.VMEM((SLOTS, depth, TILE), jnp.bfloat16),
                pltpu.VMEM((groups, SUB, local_vocab), f32),
                pltpu.VMEM((side, groups // side, SUB, local_vocab), f32),
                pltpu.VMEM((2 * side, side, own_rows // SUB, SUB, local_vocab), f32),
                pltpu.VMEM((rows, LANES), f32),
                pltpu.VMEM((rows, LANES), f32),
                pltpu.VMEM((TILE, TILE), jnp.bfloat16),
                pltpu.VMEM((rows, LANES), f32),
                pltpu.VMEM((n, SUB, LANES), f32),
                pltpu.VMEM((n, SUB, LANES), f32),
                pltpu.VMEM((own_rows // SUB, n, SUB, LANES), f32),
                pltpu.VMEM((own_rows // SUB, n, SUB, LANES), f32),
                pltpu.VMEM((own_rows // SUB, n, SUB, LANES), f32),
                pltpu.VMEM((own_rows // SUB, n, SUB, LANES), f32),
                pltpu.VMEM((1, LANES), f32),
                pltpu.VMEM((n, 1, LANES), f32),
                pltpu.SemaphoreType.DMA,
                pltpu.SemaphoreType.DMA((SLOTS,)),
                pltpu.SemaphoreType.DMA,
                pltpu.SemaphoreType.DMA((tiles + 1,)),
                pltpu.SemaphoreType.DMA,
                pltpu.SemaphoreType.DMA((tiles + 1,)),
                pltpu.SemaphoreType.DMA,
                pltpu.SemaphoreType.DMA,
                pltpu.SemaphoreType.DMA,
                pltpu.SemaphoreType.DMA,
            ],
            compiler_params=pltpu.CompilerParams(collective_id=0, has_side_effects=True, vmem_limit_bytes=54 << 20),
            name="head_cdf",
        )(hidden, w_local, inv_temp, target_ids)
        return pl.pallas_call(
            store_kernel,
            out_shape=(
                jax.ShapeDtypeStruct(table.shape, f32),
                jax.ShapeDtypeStruct(picked.shape, f32),
            ),
            in_specs=[pl.BlockSpec(memory_space=pltpu.VMEM)] * 2,
            out_specs=(pl.BlockSpec(memory_space=pltpu.HBM), pl.BlockSpec(memory_space=pltpu.HBM)),
            scratch_shapes=[pltpu.SemaphoreType.DMA((STORES,)), pltpu.SemaphoreType.DMA],
            compiler_params=pltpu.CompilerParams(vmem_limit_bytes=20 << 20),
            name="store_table",
        )(table, picked)

    return jax.shard_map(
        local_step,
        mesh=mesh,
        in_specs=(P("dp", None), P(None, "vp"), P("dp"), P("dp")),
        out_specs=(P(("dp", "vp"), None), P("dp")),
        check_vma=False,
    )
```

```python
import functools
import math

import jax
import jax.numpy as jnp
from jax import lax
from jax.experimental import pallas as pl
from jax.experimental.pallas import tpu as pltpu
from jax.sharding import PartitionSpec as P

MESH = pl.DeviceIdType.MESH
SUB = 4
LANES = 128
TILE = 256
HALF = TILE // 2
SLOTS = 3
PARTS = 4
AHEAD = 4
STORES = 8
LOW = -3.0e38


def kernel(n, hid_hbm, w_hbm, inv_ref, tgt_ref, out_ref, pick_ref, hid, wbuf, send, mid, recv, invcol, tcol, tri, stat,
           stat_out, stat_in, scale, offset, scale_b, offset_b, tval, tall, hsem, wsem, one_ss, one_rs, two_ss, two_rs,
           stat_ss, stat_rs, t_ss, t_rs):
    me = lax.axis_index("vp")
    rows, depth = hid.shape
    local_vocab = w_hbm.shape[1]
    tiles = local_vocab // TILE
    own_groups = rows // n // SUB
    width = 2 * tiles + 8
    side = math.isqrt(n // 2)
    core, x, y = me % 2, (me // 2) % side, me // (2 * side)
    a = x + core * (y - x)
    b = y + core * (x - y)

    def device(a_, b_, core_):
        row = b_ + core * (a_ - b_)
        col = a_ + core * (b_ - a_)
        return {"vp": (row * side + col) * 2 + core_}

    slab = 2 * side * own_groups

    def w_start(t):
        cols = pl.ds(pl.multiple_of(t * TILE, TILE), TILE)
        for p in range(PARTS):
            part = pl.ds(p * (depth // PARTS), depth // PARTS)
            pltpu.make_async_copy(w_hbm.at[part, cols], wbuf.at[t % SLOTS, part], wsem.at[t % SLOTS]).start()

    for p in range(PARTS):
        part = pl.ds(p * (rows // PARTS), rows // PARTS)
        pltpu.make_async_copy(hid_hbm.at[part], hid.at[part], hsem).start()
    w_start(jnp.int32(0))

    barrier = pltpu.get_barrier_semaphore()

    def knock(d, c):
        pl.semaphore_signal(barrier, inc=1, device_id={"vp": lax.rem(me + d, n)}, device_id_type=MESH)
        return c

    lax.fori_loop(1, n, knock, 0)

    eye = lax.broadcasted_iota(jnp.int32, (LANES, LANES), 0) == lax.broadcasted_iota(jnp.int32, (LANES, LANES), 1)
    shard_start = (me * local_vocab).astype(jnp.float32)
    for q in range(rows // LANES):
        cut = slice(q * LANES, (q + 1) * LANES)
        for src, dst, base in ((inv_ref, invcol, 0.0), (tgt_ref, tcol, shard_start)):
            seg = jnp.broadcast_to(src[cut].reshape(1, LANES).astype(jnp.float32), (LANES, LANES))
            col = jnp.sum(jnp.where(eye, seg, 0.0), axis=1, keepdims=True) - base
            dst[cut, :] = jnp.broadcast_to(col, (LANES, LANES))
    tri[...] = (lax.broadcasted_iota(jnp.int32, (TILE, TILE), 0) <= lax.broadcasted_iota(jnp.int32, (TILE, TILE), 1)).astype(jnp.float32).astype(jnp.bfloat16)
    stat[...] = jnp.zeros_like(stat)

    def columns(t):
        return pl.ds(pl.multiple_of(t * TILE, TILE), TILE)

    def round_columns(r, part):
        if part is None:
            return columns(r), r
        start = (tiles - 1) * TILE + part * HALF
        return pl.ds(start, HALF), tiles - 1 + part

    def first_leg(r, half=None):
        cols, k = round_columns(r, half)
        for hop in (1, side - 1, *range(2, side - 1)):
            to = (a + hop) % side
            pltpu.make_async_remote_copy(
                src_ref=send.at[pl.ds(to * slab, slab), :, cols],
                dst_ref=mid.at[a, :, :, cols],
                send_sem=one_ss,
                recv_sem=one_rs.at[k],
                device_id=device(to, b, core),
                device_id_type=MESH,
            ).start()

    def second_leg(r, half=None):
        cols, k = round_columns(r, half)
        part = mid.at[pl.ds(0, side - 1), :, :, pl.ds(0, TILE if half is None else HALF)]
        pltpu.make_async_copy(part, part, one_rs.at[k]).wait()

        def onward(to, core_):
            pltpu.make_async_remote_copy(
                src_ref=mid.at[:, pl.ds((to * 2 + core_) * own_groups, own_groups), :, cols],
                dst_ref=recv.at[core * side + b, :, :, :, cols],
                send_sem=two_ss,
                recv_sem=two_rs.at[k],
                device_id=device(a, to, core_),
                device_id_type=MESH,
            ).start()

        for hop in (1, side - 1, *range(2, side - 1)):
            for core_ in range(2):
                onward((b + hop) % side, core_)
        onward(b, 1 - core)
        recv[core * side + b, :, :, :, cols] = mid[:, pl.ds((b * 2 + core) * own_groups, own_groups), :, cols]

    def compute_tile(t):
        pltpu.make_async_copy(wbuf.at[t % SLOTS], wbuf.at[t % SLOTS], wsem.at[t % SLOTS]).wait()

        @pl.when(t == 0)
        def _():
            w_start(t + 1)

        @pl.when(t + 2 < tiles)
        def _():
            w_start(t + 2)

        z = jnp.dot(hid[...], wbuf[t % SLOTS], preferred_element_type=jnp.float32)
        z = z * jnp.concatenate([invcol[...]] * (TILE // LANES), axis=1)
        top = jnp.max(z, axis=1, keepdims=True)
        e = jnp.exp(z - top)
        hi = e.astype(jnp.bfloat16)
        rest = e - hi.astype(jnp.float32)
        more = rest.astype(jnp.bfloat16)
        low = (rest - more.astype(jnp.float32)).astype(jnp.bfloat16)
        upto = tri[...]
        run = jnp.dot(low, upto, preferred_element_type=jnp.float32)
        run = run + jnp.dot(more, upto, preferred_element_type=jnp.float32)
        run = run + jnp.dot(hi, upto, preferred_element_type=jnp.float32)
        cols = columns(t)
        for k in range(rows // SUB):
            owner, g = divmod(k, own_groups)
            oy, ox, oc = owner // (2 * side), (owner // 2) % side, owner % 2
            x_first, y_first = ((ox * side + oy) * 2 + oc) * own_groups + g, ((oy * side + ox) * 2 + oc) * own_groups + g
            send[x_first + core * (y_first - x_first), :, cols] = run[k * SUB : (k + 1) * SUB]
        at = lax.broadcasted_iota(jnp.int32, (rows, TILE), 1).astype(jnp.float32) + (t * TILE).astype(jnp.float32)
        tc = jnp.concatenate([tcol[...]] * (TILE // LANES), axis=1)
        hit = jnp.sum(jnp.where(at == tc, run, 0.0), axis=1, keepdims=True)
        lane = lax.broadcasted_iota(jnp.int32, (rows, LANES), 1)
        st = stat[...]
        st = jnp.where(lane == t, top, st)
        st = jnp.where(lane == tiles + t, run[:, TILE - 1 :], st)
        st = jnp.where(lane == 2 * tiles, st + hit, st)
        stat[...] = st
        mid[a, :, :, cols] = send[pl.ds(a * slab, slab), :, cols]

    def send_statistics():
        lane8 = lax.broadcasted_iota(jnp.int32, (rows, LANES), 1)
        stat[...] = jnp.where(lane8 == 2 * tiles + 1, tcol[...], stat[...])
        for i in range(n):
            block = None
            for g in range(own_groups):
                k = i * own_groups + g
                part = stat[k * SUB : (k + 1) * SUB, :]
                part = part if g == 0 else pltpu.roll(part, g * width, 1)
                block = part if block is None else block + part
            stat_out[i] = block
        stat_in[me] = stat_out[me]

        def go(d, c):
            peer = lax.rem(me + d, n)
            pltpu.make_async_remote_copy(
                src_ref=stat_out.at[peer], dst_ref=stat_in.at[me], send_sem=stat_ss, recv_sem=stat_rs,
                device_id={"vp": peer}, device_id_type=MESH,
            ).start()
            return c

        lax.fori_loop(1, n, go, 0)

    def take_statistics():
        pltpu.make_async_copy(stat_in.at[pl.ds(0, n - 1)], stat_in.at[pl.ds(0, n - 1)], stat_rs).wait()
        lane = lax.broadcasted_iota(jnp.int32, (n, SUB, LANES), 2)
        first = lane < tiles
        lane4 = lax.broadcasted_iota(jnp.int32, (SUB, LANES), 1)
        row4 = lax.broadcasted_iota(jnp.int32, (SUB, LANES), 0)
        line = jnp.zeros((SUB, LANES), jnp.float32)
        for g in range(own_groups):
            got = stat_in[...]
            if g:
                got = pltpu.roll(got, LANES - g * width, 2)
            tops = jnp.where(first, got, LOW)
            top = jnp.max(jnp.max(tops, axis=0, keepdims=True), axis=2, keepdims=True)
            weight = jnp.where(first, jnp.exp(tops - top), 0.0)
            mass = weight * jnp.where(first, pltpu.roll(got, LANES - tiles, 2), 0.0)
            upto = mass
            shift = 1
            while shift < tiles:
                upto = upto + jnp.where(lane >= shift, pltpu.roll(upto, shift, 2), 0.0)
                shift *= 2
            before = jnp.where(lane >= 1, pltpu.roll(upto, 1, 2), 0.0)
            shard = jnp.sum(mass, axis=2, keepdims=True)
            start = jnp.zeros((1, SUB, 1), jnp.float32)
            starts = []
            for s in range(n):
                starts.append(start)
                start = start + shard[s : s + 1]
            inv = 1.0 / start
            sc = weight * inv
            of = (before + jnp.concatenate(starts, axis=0)) * inv
            scale[g] = sc
            offset[g] = of
            picked = jnp.broadcast_to(got[:, :, 2 * tiles : 2 * tiles + 1], got.shape)
            target = jnp.broadcast_to(got[:, :, 2 * tiles + 1 : 2 * tiles + 2], got.shape)
            lo = (lane * TILE).astype(jnp.float32)
            hit = first & (target >= lo) & (target < lo + float(TILE))
            val = jnp.where(hit, sc * picked + of, 0.0)
            val = jnp.sum(jnp.sum(val, axis=0), axis=1, keepdims=True)
            line = jnp.where(lane4 == row4 + g * SUB, val, line)
        line = jnp.sum(line, axis=0, keepdims=True)
        tval[...] = line
        tall[me] = line

        def go(d, c):
            pltpu.make_async_remote_copy(
                src_ref=tval, dst_ref=tall.at[me], send_sem=t_ss, recv_sem=t_rs,
                device_id={"vp": lax.rem(me + d, n)}, device_id_type=MESH,
            ).start()
            return c

        lax.fori_loop(1, n, go, 0)

    def widen(t):
        for g in range(own_groups):
            for ref, wide in ((scale, scale_b), (offset, offset_b)):
                v = ref[g]
                wide[g] = jnp.broadcast_to(v[:, :, :1], v.shape)
                ref[g] = pltpu.roll(v, LANES - 1, 2)

    def finish_round(r, half=None):
        size = TILE if half is None else HALF
        base = r * TILE if half is None else (tiles - 1) * TILE + half * HALF
        if not half:
            widen(r)
        part = recv.at[pl.ds(0, 2 * side - 1), :, :, :, pl.ds(0, size)]
        pltpu.make_async_copy(part, part, two_rs.at[r if half is None else tiles - 1 + half]).wait()

        def one(q, c):
            relay, u = q // side, q % side
            core_, v = relay // side, relay % side
            row = v + core_ * (u - v)
            col = u + core_ * (v - u)
            s = (row * side + col) * 2 + core_
            for g in range(own_groups):
                sc, of = scale_b[g, s], offset_b[g, s]
                for h in range(size // LANES):
                    here = pl.ds(pl.multiple_of(base + h * LANES, LANES), LANES)
                    cols = pl.ds(pl.multiple_of(s * local_vocab + base + h * LANES, LANES), LANES)
                    out_ref[g * SUB : (g + 1) * SUB, cols] = recv[relay, u, g, :, here] * sc + of
            return c

        lax.fori_loop(0, n, one, 0, unroll=4)

    pltpu.make_async_copy(hid, hid, hsem).wait()

    def early(t, c):
        compute_tile(t)

        @pl.when(t == 0)
        def _():
            pl.semaphore_wait(barrier, n - 1)
            first_leg(t)

        @pl.when((t >= 1) & (t < AHEAD))
        def _():
            first_leg(t)

        @pl.when((t >= AHEAD) & ((t - AHEAD) % 2 == 1))
        def _():
            first_leg(AHEAD + (t - AHEAD) // 2)

        @pl.when((t >= AHEAD + 2) & ((t - AHEAD) % 2 == 0))
        def _():
            second_leg((t - AHEAD) // 2 - 1)

        return c

    lax.fori_loop(0, tiles, early, 0)
    send_statistics()

    lead = AHEAD + 1
    next_one, next_two = AHEAD + (tiles - AHEAD) // 2, (tiles - 1 - AHEAD) // 2
    for k in range(next_one, next_two + lead):
        first_leg(jnp.int32(k))
    take_at = next_two + 3

    def late(k, c):
        first_leg(k + lead)

        @pl.when(k == take_at)
        def _():
            take_statistics()

        second_leg(k)

        @pl.when(k >= take_at)
        def _():
            for m in range(3):
                finish_round((k - take_at) * 3 + m)

        return c

    stop = tiles - 1 - lead
    lax.fori_loop(next_two, stop, late, 0)
    first_leg(None, 0)
    first_leg(None, 1)

    def finish_to(lo, hi):
        def body(r, c):
            finish_round(r)
            return c

        lax.fori_loop(lo, hi, body, 0)

    ready = (stop - take_at) * 3

    def ending(k, c):
        second_leg(k)
        finish_round(k - stop + ready)
        return c

    lax.fori_loop(stop, tiles - 1, ending, 0)
    second_leg(None, 0)
    second_leg(None, 1)
    finish_to(tiles - 1 - stop + ready, tiles - 1)
    pltpu.make_async_copy(tall.at[pl.ds(0, n - 1)], tall.at[pl.ds(0, n - 1)], t_rs).wait()
    own_rows = own_groups * SUB
    lane1 = lax.broadcasted_iota(jnp.int32, (1, LANES), 1)
    acc = [jnp.zeros((1, LANES), jnp.float32) for _ in range(rows // LANES)]
    for s in range(n):
        q, off = divmod(s * own_rows, LANES)
        line = tall[s]
        line = pltpu.roll(line, off, 1) if off else line
        acc[q] = acc[q] + jnp.where(lane1 >= off, line, 0.0)
        if off + own_rows > LANES:
            acc[q + 1] = acc[q + 1] + jnp.where(lane1 < off, line, 0.0)
    for q in range(rows // LANES):
        pick_ref[q * LANES : (q + 1) * LANES] = acc[q].reshape(LANES)

    finish_round(tiles - 1, 0)
    finish_round(tiles - 1, 1)

    pltpu.make_async_copy(mid.at[pl.ds(0, side - 1)], mid.at[pl.ds(0, side - 1)], one_ss).wait()
    pltpu.make_async_copy(recv.at[pl.ds(0, 2 * side - 1)], recv.at[pl.ds(0, 2 * side - 1)], two_ss).wait()
    pltpu.make_async_copy(stat_in.at[pl.ds(0, n - 1)], stat_in.at[pl.ds(0, n - 1)], stat_ss).wait()
    pltpu.make_async_copy(tall.at[pl.ds(0, n - 1)], tall.at[pl.ds(0, n - 1)], t_ss).wait()


def store_kernel(table, picked, table_out, picked_out, sem, small_sem):
    width = table.shape[1] // STORES
    copies = [pltpu.make_async_copy(picked, picked_out, small_sem)]
    for i in range(STORES):
        cols = pl.ds(i * width, width)
        for k, rows in enumerate((pl.ds(0, 8), pl.ds(8, table.shape[0] - 8))):
            copies.append(pltpu.make_async_copy(table.at[rows, cols], table_out.at[rows, cols], sem.at[i, k]))
    for copy in copies:
        copy.start()
    for copy in copies:
        copy.wait()


def solution(mesh):
    n = mesh.shape["vp"]
    side = math.isqrt(n // 2)

    def local_step(hidden, w_local, inv_temp, target_ids):
        rows, depth = hidden.shape
        local_vocab = w_local.shape[1]
        tiles = local_vocab // TILE
        groups = rows // SUB
        own_rows = rows // n
        f32 = jnp.float32
        table, picked = pl.pallas_call(
            functools.partial(kernel, n),
            out_shape=(
                pltpu.VMEM((own_rows, n * local_vocab), f32),
                pltpu.VMEM((rows,), f32),
            ),
            in_specs=[
                pl.BlockSpec(memory_space=pltpu.HBM),
                pl.BlockSpec(memory_space=pltpu.HBM),
                pl.BlockSpec(memory_space=pltpu.VMEM),
                pl.BlockSpec(memory_space=pltpu.VMEM),
            ],
            out_specs=(pl.BlockSpec(memory_space=pltpu.VMEM), pl.BlockSpec(memory_space=pltpu.VMEM)),
            scratch_shapes=[
                pltpu.VMEM((rows, depth), jnp.bfloat16),
                pltpu.VMEM((SLOTS, depth, TILE), jnp.bfloat16),
                pltpu.VMEM((groups, SUB, local_vocab), f32),
                pltpu.VMEM((side, groups // side, SUB, local_vocab), f32),
                pltpu.VMEM((2 * side, side, own_rows // SUB, SUB, local_vocab), f32),
                pltpu.VMEM((rows, LANES), f32),
                pltpu.VMEM((rows, LANES), f32),
                pltpu.VMEM((TILE, TILE), jnp.bfloat16),
                pltpu.VMEM((rows, LANES), f32),
                pltpu.VMEM((n, SUB, LANES), f32),
                pltpu.VMEM((n, SUB, LANES), f32),
                pltpu.VMEM((own_rows // SUB, n, SUB, LANES), f32),
                pltpu.VMEM((own_rows // SUB, n, SUB, LANES), f32),
                pltpu.VMEM((own_rows // SUB, n, SUB, LANES), f32),
                pltpu.VMEM((own_rows // SUB, n, SUB, LANES), f32),
                pltpu.VMEM((1, LANES), f32),
                pltpu.VMEM((n, 1, LANES), f32),
                pltpu.SemaphoreType.DMA,
                pltpu.SemaphoreType.DMA((SLOTS,)),
                pltpu.SemaphoreType.DMA,
                pltpu.SemaphoreType.DMA((tiles + 1,)),
                pltpu.SemaphoreType.DMA,
                pltpu.SemaphoreType.DMA((tiles + 1,)),
                pltpu.SemaphoreType.DMA,
                pltpu.SemaphoreType.DMA,
                pltpu.SemaphoreType.DMA,
                pltpu.SemaphoreType.DMA,
            ],
            compiler_params=pltpu.CompilerParams(collective_id=0, has_side_effects=True, vmem_limit_bytes=54 << 20),
            name="head_cdf",
        )(hidden, w_local, inv_temp, target_ids)
        return pl.pallas_call(
            store_kernel,
            out_shape=(
                jax.ShapeDtypeStruct(table.shape, f32),
                jax.ShapeDtypeStruct(picked.shape, f32),
            ),
            in_specs=[pl.BlockSpec(memory_space=pltpu.VMEM)] * 2,
            out_specs=(pl.BlockSpec(memory_space=pltpu.HBM), pl.BlockSpec(memory_space=pltpu.HBM)),
            scratch_shapes=[pltpu.SemaphoreType.DMA((STORES, 2)), pltpu.SemaphoreType.DMA],
            compiler_params=pltpu.CompilerParams(vmem_limit_bytes=20 << 20),
            name="store_table",
        )(table, picked)

    return jax.shard_map(
        local_step,
        mesh=mesh,
        in_specs=(P("dp", None), P(None, "vp"), P("dp"), P("dp")),
        out_specs=(P(("dp", "vp"), None), P("dp")),
        check_vma=False,
    )
```

```python
import functools
import math

import jax
import jax.numpy as jnp
from jax import lax
from jax.experimental import pallas as pl
from jax.experimental.pallas import tpu as pltpu
from jax.sharding import PartitionSpec as P

MESH = pl.DeviceIdType.MESH
SUB = 4
LANES = 128
TILE = 256
HALF = TILE // 2
SLOTS = 3
PARTS = 4
STORES = 8
LOW = -3.0e38


def kernel(n, hid_hbm, w_hbm, inv_ref, tgt_ref, out_ref, pick_ref, hid, wbuf, send, mid, recv, invcol, tcol, tri, stat,
           stat_out, stat_in, scale, offset, scale_b, offset_b, tval, tall, hsem, fsem, wsem, one_ss, one_rs, two_ss, two_rs,
           stat_ss, stat_rs, t_ss, t_rs):
    me = lax.axis_index("vp")
    rows, depth = hid.shape
    local_vocab = w_hbm.shape[1]
    tiles = local_vocab // TILE
    own_groups = rows // n // SUB
    width = 2 * tiles + 8
    side = math.isqrt(n // 2)
    core, x, y = me % 2, (me // 2) % side, me // (2 * side)
    a = x + core * (y - x)
    b = y + core * (x - y)

    def device(a_, b_, core_):
        row = b_ + core * (a_ - b_)
        col = a_ + core * (b_ - a_)
        return {"vp": (row * side + col) * 2 + core_}

    slab = 2 * side * own_groups

    def w_start(t):
        cols = pl.ds(pl.multiple_of(t * TILE, TILE), TILE)
        for p in range(PARTS):
            part = pl.ds(p * (depth // PARTS), depth // PARTS)
            pltpu.make_async_copy(w_hbm.at[part, cols], wbuf.at[t % SLOTS, part], wsem.at[t % SLOTS]).start()

    def depth_part(p):
        return pl.ds(p * (depth // PARTS), depth // PARTS)

    def first_loads(p):
        part = depth_part(p)
        return (
            pltpu.make_async_copy(hid_hbm.at[:, part], hid.at[:, part], hsem.at[p]),
            pltpu.make_async_copy(w_hbm.at[part, pl.ds(0, TILE)], wbuf.at[0, part], fsem.at[p]),
        )

    for p in range(PARTS):
        for copy in first_loads(p):
            copy.start()

    barrier = pltpu.get_barrier_semaphore()

    def knock(d, c):
        pl.semaphore_signal(barrier, inc=1, device_id={"vp": lax.rem(me + d, n)}, device_id_type=MESH)
        return c

    lax.fori_loop(1, n, knock, 0)

    eye = lax.broadcasted_iota(jnp.int32, (LANES, LANES), 0) == lax.broadcasted_iota(jnp.int32, (LANES, LANES), 1)
    shard_start = (me * local_vocab).astype(jnp.float32)
    for q in range(rows // LANES):
        cut = slice(q * LANES, (q + 1) * LANES)
        for src, dst, base in ((inv_ref, invcol, 0.0), (tgt_ref, tcol, shard_start)):
            seg = jnp.broadcast_to(src[cut].reshape(1, LANES).astype(jnp.float32), (LANES, LANES))
            col = jnp.sum(jnp.where(eye, seg, 0.0), axis=1, keepdims=True) - base
            dst[cut, :] = jnp.broadcast_to(col, (LANES, LANES))
    tri[...] = (lax.broadcasted_iota(jnp.int32, (TILE, TILE), 0) <= lax.broadcasted_iota(jnp.int32, (TILE, TILE), 1)).astype(jnp.float32).astype(jnp.bfloat16)
    stat[...] = jnp.zeros_like(stat)

    def columns(t):
        return pl.ds(pl.multiple_of(t * TILE, TILE), TILE)

    def round_columns(r, part):
        if part is None:
            return columns(r), r
        start = (tiles - 1) * TILE + part * HALF
        return pl.ds(start, HALF), tiles - 1 + part

    def first_leg(r, half=None):
        cols, k = round_columns(r, half)
        for hop in (1, side - 1, *range(2, side - 1)):
            to = (a + hop) % side
            pltpu.make_async_remote_copy(
                src_ref=send.at[pl.ds(to * slab, slab), :, cols],
                dst_ref=mid.at[a, :, :, cols],
                send_sem=one_ss,
                recv_sem=one_rs.at[k],
                device_id=device(to, b, core),
                device_id_type=MESH,
            ).start()

    def second_leg(r, half=None):
        cols, k = round_columns(r, half)
        part = mid.at[pl.ds(0, side - 1), :, :, pl.ds(0, TILE if half is None else HALF)]
        pltpu.make_async_copy(part, part, one_rs.at[k]).wait()

        def onward(to, core_):
            pltpu.make_async_remote_copy(
                src_ref=mid.at[:, pl.ds((to * 2 + core_) * own_groups, own_groups), :, cols],
                dst_ref=recv.at[core * side + b, :, :, :, cols],
                send_sem=two_ss,
                recv_sem=two_rs.at[k],
                device_id=device(a, to, core_),
                device_id_type=MESH,
            ).start()

        for hop in (1, side - 1, *range(2, side - 1)):
            for core_ in range(2):
                onward((b + hop) % side, core_)
        onward(b, 1 - core)
        recv[core * side + b, :, :, :, cols] = mid[:, pl.ds((b * 2 + core) * own_groups, own_groups), :, cols]

    def compute_tile(t, send_now=None):
        if send_now:
            z = None
            for p in range(PARTS):
                for copy in first_loads(p):
                    copy.wait()
                if p == PARTS - 1:
                    w_start(jnp.int32(1))
                    w_start(jnp.int32(2))
                term = jnp.dot(hid[:, depth_part(p)], wbuf[0, depth_part(p)], preferred_element_type=jnp.float32)
                z = term if z is None else z + term
        else:
            pltpu.make_async_copy(wbuf.at[t % SLOTS], wbuf.at[t % SLOTS], wsem.at[t % SLOTS]).wait()

            @pl.when(t + 2 < tiles)
            def _():
                w_start(t + 2)

            z = jnp.dot(hid[...], wbuf[t % SLOTS], preferred_element_type=jnp.float32)
        z = z * jnp.concatenate([invcol[...]] * (TILE // LANES), axis=1)
        top = jnp.max(z, axis=1, keepdims=True)
        e = jnp.exp(z - top)
        hi = e.astype(jnp.bfloat16)
        rest = e - hi.astype(jnp.float32)
        more = rest.astype(jnp.bfloat16)
        low = (rest - more.astype(jnp.float32)).astype(jnp.bfloat16)
        upto = tri[...]
        run = jnp.dot(low, upto, preferred_element_type=jnp.float32)
        run = run + jnp.dot(more, upto, preferred_element_type=jnp.float32)
        run = run + jnp.dot(hi, upto, preferred_element_type=jnp.float32)
        cols = columns(t)
        for k in range(rows // SUB):
            owner, g = divmod(k, own_groups)
            oy, ox, oc = owner // (2 * side), (owner // 2) % side, owner % 2
            x_first, y_first = ((ox * side + oy) * 2 + oc) * own_groups + g, ((oy * side + ox) * 2 + oc) * own_groups + g
            send[x_first + core * (y_first - x_first), :, cols] = run[k * SUB : (k + 1) * SUB]
        mid[a, :, :, cols] = send[pl.ds(a * slab, slab), :, cols]
        if send_now:
            send_now()
        at = lax.broadcasted_iota(jnp.int32, (rows, TILE), 1).astype(jnp.float32) + (t * TILE).astype(jnp.float32)
        tc = jnp.concatenate([tcol[...]] * (TILE // LANES), axis=1)
        hit = jnp.sum(jnp.where(at == tc, run, 0.0), axis=1, keepdims=True)
        lane = lax.broadcasted_iota(jnp.int32, (rows, LANES), 1)
        st = stat[...]
        st = jnp.where(lane == t, top, st)
        st = jnp.where(lane == tiles + t, run[:, TILE - 1 :], st)
        st = jnp.where(lane == 2 * tiles, st + hit, st)
        stat[...] = st

    def send_statistics():
        lane8 = lax.broadcasted_iota(jnp.int32, (rows, LANES), 1)
        stat[...] = jnp.where(lane8 == 2 * tiles + 1, tcol[...], stat[...])
        for i in range(n):
            block = None
            for g in range(own_groups):
                k = i * own_groups + g
                part = stat[k * SUB : (k + 1) * SUB, :]
                part = part if g == 0 else pltpu.roll(part, g * width, 1)
                block = part if block is None else block + part
            stat_out[i] = block
        stat_in[me] = stat_out[me]

        def go(d, c):
            peer = lax.rem(me + d, n)
            pltpu.make_async_remote_copy(
                src_ref=stat_out.at[peer], dst_ref=stat_in.at[me], send_sem=stat_ss, recv_sem=stat_rs,
                device_id={"vp": peer}, device_id_type=MESH,
            ).start()
            return c

        lax.fori_loop(1, n, go, 0)

    def take_statistics():
        pltpu.make_async_copy(stat_in.at[pl.ds(0, n - 1)], stat_in.at[pl.ds(0, n - 1)], stat_rs).wait()
        lane = lax.broadcasted_iota(jnp.int32, (n, SUB, LANES), 2)
        first = lane < tiles
        lane4 = lax.broadcasted_iota(jnp.int32, (SUB, LANES), 1)
        row4 = lax.broadcasted_iota(jnp.int32, (SUB, LANES), 0)
        line = jnp.zeros((SUB, LANES), jnp.float32)
        for g in range(own_groups):
            got = stat_in[...]
            if g:
                got = pltpu.roll(got, LANES - g * width, 2)
            tops = jnp.where(first, got, LOW)
            top = jnp.max(jnp.max(tops, axis=0, keepdims=True), axis=2, keepdims=True)
            weight = jnp.where(first, jnp.exp(tops - top), 0.0)
            mass = weight * jnp.where(first, pltpu.roll(got, LANES - tiles, 2), 0.0)
            upto = mass
            shift = 1
            while shift < tiles:
                upto = upto + jnp.where(lane >= shift, pltpu.roll(upto, shift, 2), 0.0)
                shift *= 2
            before = jnp.where(lane >= 1, pltpu.roll(upto, 1, 2), 0.0)
            shard = jnp.sum(mass, axis=2, keepdims=True)
            start = jnp.zeros((1, SUB, 1), jnp.float32)
            starts = []
            for s in range(n):
                starts.append(start)
                start = start + shard[s : s + 1]
            inv = 1.0 / start
            sc = weight * inv
            of = (before + jnp.concatenate(starts, axis=0)) * inv
            scale[g] = sc
            offset[g] = of
            picked = jnp.broadcast_to(got[:, :, 2 * tiles : 2 * tiles + 1], got.shape)
            target = jnp.broadcast_to(got[:, :, 2 * tiles + 1 : 2 * tiles + 2], got.shape)
            lo = (lane * TILE).astype(jnp.float32)
            hit = first & (target >= lo) & (target < lo + float(TILE))
            val = jnp.where(hit, sc * picked + of, 0.0)
            val = jnp.sum(jnp.sum(val, axis=0), axis=1, keepdims=True)
            line = jnp.where(lane4 == row4 + g * SUB, val, line)
        line = jnp.sum(line, axis=0, keepdims=True)
        tval[...] = line
        tall[me] = line

        def go(d, c):
            pltpu.make_async_remote_copy(
                src_ref=tval, dst_ref=tall.at[me], send_sem=t_ss, recv_sem=t_rs,
                device_id={"vp": lax.rem(me + d, n)}, device_id_type=MESH,
            ).start()
            return c

        lax.fori_loop(1, n, go, 0)

    def widen(t):
        for g in range(own_groups):
            for ref, wide in ((scale, scale_b), (offset, offset_b)):
                v = ref[g]
                wide[g] = jnp.broadcast_to(v[:, :, :1], v.shape)
                ref[g] = pltpu.roll(v, LANES - 1, 2)

    def finish_round(r, half=None):
        size = TILE if half is None else HALF
        base = r * TILE if half is None else (tiles - 1) * TILE + half * HALF
        if not half:
            widen(r)
        part = recv.at[pl.ds(0, 2 * side - 1), :, :, :, pl.ds(0, size)]
        pltpu.make_async_copy(part, part, two_rs.at[r if half is None else tiles - 1 + half]).wait()

        def one(q, c):
            relay, u = q // side, q % side
            core_, v = relay // side, relay % side
            row = v + core_ * (u - v)
            col = u + core_ * (v - u)
            s = (row * side + col) * 2 + core_
            for g in range(own_groups):
                sc, of = scale_b[g, s], offset_b[g, s]
                for h in range(size // LANES):
                    here = pl.ds(pl.multiple_of(base + h * LANES, LANES), LANES)
                    cols = pl.ds(pl.multiple_of(s * local_vocab + base + h * LANES, LANES), LANES)
                    out_ref[g * SUB : (g + 1) * SUB, cols] = recv[relay, u, g, :, here] * sc + of
            return c

        lax.fori_loop(0, n, one, 0, unroll=4)

    def first_send():
        pl.semaphore_wait(barrier, n - 1)
        first_leg(jnp.int32(0))

    compute_tile(jnp.int32(0), first_send)

    def early(t, c):
        compute_tile(t)

        @pl.when(t == 1)
        def _():
            first_leg(t)

        @pl.when((t >= 2) & (t % 2 == 0))
        def _():
            first_leg(t // 2 + 1)

        @pl.when((t >= 3) & (t % 2 == 1))
        def _():
            second_leg((t - 3) // 2)

        return c

    lax.fori_loop(1, tiles, early, 0)
    send_statistics()

    next_one, next_two = tiles // 2 + 1, tiles // 2 - 1
    first_leg(jnp.int32(next_one))
    lead = next_one + 1 - next_two
    take_at = next_two + 3

    def late(k, c):
        first_leg(k + lead)

        @pl.when(k == take_at)
        def _():
            take_statistics()

        second_leg(k)

        @pl.when(k >= take_at)
        def _():
            for m in range(3):
                finish_round((k - take_at) * 3 + m)

        return c

    stop = tiles - 1 - lead
    lax.fori_loop(next_two, stop, late, 0)
    first_leg(None, 0)
    first_leg(None, 1)

    def finish_to(lo, hi):
        def body(r, c):
            finish_round(r)
            return c

        lax.fori_loop(lo, hi, body, 0)

    def ending(k, c):
        second_leg(k)
        finish_round((k - stop) * 2 + (stop - take_at) * 3)
        finish_round((k - stop) * 2 + (stop - take_at) * 3 + 1)
        return c

    lax.fori_loop(stop, tiles - 1, ending, 0)
    second_leg(None, 0)
    second_leg(None, 1)
    finish_to((stop - take_at) * 3 + lead * 2, tiles - 1)
    pltpu.make_async_copy(tall.at[pl.ds(0, n - 1)], tall.at[pl.ds(0, n - 1)], t_rs).wait()
    own_rows = own_groups * SUB
    lane1 = lax.broadcasted_iota(jnp.int32, (1, LANES), 1)
    acc = [jnp.zeros((1, LANES), jnp.float32) for _ in range(rows // LANES)]
    for s in range(n):
        q, off = divmod(s * own_rows, LANES)
        line = tall[s]
        line = pltpu.roll(line, off, 1) if off else line
        acc[q] = acc[q] + jnp.where(lane1 >= off, line, 0.0)
        if off + own_rows > LANES:
            acc[q + 1] = acc[q + 1] + jnp.where(lane1 < off, line, 0.0)
    for q in range(rows // LANES):
        pick_ref[q * LANES : (q + 1) * LANES] = acc[q].reshape(LANES)

    finish_round(tiles - 1, 0)
    finish_round(tiles - 1, 1)

    pltpu.make_async_copy(mid.at[pl.ds(0, side - 1)], mid.at[pl.ds(0, side - 1)], one_ss).wait()
    pltpu.make_async_copy(recv.at[pl.ds(0, 2 * side - 1)], recv.at[pl.ds(0, 2 * side - 1)], two_ss).wait()
    pltpu.make_async_copy(stat_in.at[pl.ds(0, n - 1)], stat_in.at[pl.ds(0, n - 1)], stat_ss).wait()
    pltpu.make_async_copy(tall.at[pl.ds(0, n - 1)], tall.at[pl.ds(0, n - 1)], t_ss).wait()


def store_kernel(table, picked, table_out, picked_out, sem, small_sem):
    width = table.shape[1] // STORES
    copies = [pltpu.make_async_copy(picked, picked_out, small_sem)]
    for i in range(STORES):
        cols = pl.ds(i * width, width)
        copies.append(pltpu.make_async_copy(table.at[:, cols], table_out.at[:, cols], sem.at[i]))
    for copy in copies:
        copy.start()
    for copy in copies:
        copy.wait()


def solution(mesh):
    n = mesh.shape["vp"]
    side = math.isqrt(n // 2)

    def local_step(hidden, w_local, inv_temp, target_ids):
        rows, depth = hidden.shape
        local_vocab = w_local.shape[1]
        tiles = local_vocab // TILE
        groups = rows // SUB
        own_rows = rows // n
        f32 = jnp.float32
        table, picked = pl.pallas_call(
            functools.partial(kernel, n),
            out_shape=(
                pltpu.VMEM((own_rows, n * local_vocab), f32),
                pltpu.VMEM((rows,), f32),
            ),
            in_specs=[
                pl.BlockSpec(memory_space=pltpu.HBM),
                pl.BlockSpec(memory_space=pltpu.HBM),
                pl.BlockSpec(memory_space=pltpu.VMEM),
                pl.BlockSpec(memory_space=pltpu.VMEM),
            ],
            out_specs=(pl.BlockSpec(memory_space=pltpu.VMEM), pl.BlockSpec(memory_space=pltpu.VMEM)),
            scratch_shapes=[
                pltpu.VMEM((rows, depth), jnp.bfloat16),
                pltpu.VMEM((SLOTS, depth, TILE), jnp.bfloat16),
                pltpu.VMEM((groups, SUB, local_vocab), f32),
                pltpu.VMEM((side, groups // side, SUB, local_vocab), f32),
                pltpu.VMEM((2 * side, side, own_rows // SUB, SUB, local_vocab), f32),
                pltpu.VMEM((rows, LANES), f32),
                pltpu.VMEM((rows, LANES), f32),
                pltpu.VMEM((TILE, TILE), jnp.bfloat16),
                pltpu.VMEM((rows, LANES), f32),
                pltpu.VMEM((n, SUB, LANES), f32),
                pltpu.VMEM((n, SUB, LANES), f32),
                pltpu.VMEM((own_rows // SUB, n, SUB, LANES), f32),
                pltpu.VMEM((own_rows // SUB, n, SUB, LANES), f32),
                pltpu.VMEM((own_rows // SUB, n, SUB, LANES), f32),
                pltpu.VMEM((own_rows // SUB, n, SUB, LANES), f32),
                pltpu.VMEM((1, LANES), f32),
                pltpu.VMEM((n, 1, LANES), f32),
                pltpu.SemaphoreType.DMA((PARTS,)),
                pltpu.SemaphoreType.DMA((PARTS,)),
                pltpu.SemaphoreType.DMA((SLOTS,)),
                pltpu.SemaphoreType.DMA,
                pltpu.SemaphoreType.DMA((tiles + 1,)),
                pltpu.SemaphoreType.DMA,
                pltpu.SemaphoreType.DMA((tiles + 1,)),
                pltpu.SemaphoreType.DMA,
                pltpu.SemaphoreType.DMA,
                pltpu.SemaphoreType.DMA,
                pltpu.SemaphoreType.DMA,
            ],
            compiler_params=pltpu.CompilerParams(collective_id=0, has_side_effects=True, vmem_limit_bytes=54 << 20),
            name="head_cdf",
        )(hidden, w_local, inv_temp, target_ids)
        return pl.pallas_call(
            store_kernel,
            out_shape=(
                jax.ShapeDtypeStruct(table.shape, f32),
                jax.ShapeDtypeStruct(picked.shape, f32),
            ),
            in_specs=[pl.BlockSpec(memory_space=pltpu.VMEM)] * 2,
            out_specs=(pl.BlockSpec(memory_space=pltpu.HBM), pl.BlockSpec(memory_space=pltpu.HBM)),
            scratch_shapes=[pltpu.SemaphoreType.DMA((STORES,)), pltpu.SemaphoreType.DMA],
            compiler_params=pltpu.CompilerParams(vmem_limit_bytes=20 << 20),
            name="store_table",
        )(table, picked)

    return jax.shard_map(
        local_step,
        mesh=mesh,
        in_specs=(P("dp", None), P(None, "vp"), P("dp"), P("dp")),
        out_specs=(P(("dp", "vp"), None), P("dp")),
        check_vma=False,
    )
```

```python
import functools
import math

import jax
import jax.numpy as jnp
from jax import lax
from jax.experimental import pallas as pl
from jax.experimental.pallas import tpu as pltpu
from jax.sharding import PartitionSpec as P

MESH = pl.DeviceIdType.MESH
SUB = 4
LANES = 128
TILE = 256
HALF = TILE // 2
SLOTS = 3
PARTS = 4
STORES = 8
LOW = -3.0e38


def kernel(n, hid_hbm, w_hbm, inv_ref, tgt_ref, out_ref, pick_ref, hid, wbuf, send, mid, recv, invcol, tcol, tri, stat,
           stat_out, stat_in, scale, offset, scale_b, offset_b, tval, tall, hsem, fsem, wsem, one_ss, one_rs, two_ss, two_rs,
           stat_ss, stat_rs, t_ss, t_rs):
    me = lax.axis_index("vp")
    rows, depth = hid.shape
    local_vocab = w_hbm.shape[1]
    tiles = local_vocab // TILE
    own_groups = rows // n // SUB
    width = 2 * tiles + 8
    side = math.isqrt(n // 2)
    core, x, y = me % 2, (me // 2) % side, me // (2 * side)
    a = x + core * (y - x)
    b = y + core * (x - y)

    def device(a_, b_, core_):
        row = b_ + core * (a_ - b_)
        col = a_ + core * (b_ - a_)
        return {"vp": (row * side + col) * 2 + core_}

    slab = 2 * side * own_groups

    def w_start(t):
        cols = pl.ds(pl.multiple_of(t * TILE, TILE), TILE)
        for p in range(PARTS):
            part = pl.ds(p * (depth // PARTS), depth // PARTS)
            pltpu.make_async_copy(w_hbm.at[part, cols], wbuf.at[t % SLOTS, part], wsem.at[t % SLOTS]).start()

    def depth_part(p):
        return pl.ds(p * (depth // PARTS), depth // PARTS)

    def first_loads(p):
        part = depth_part(p)
        return (
            pltpu.make_async_copy(hid_hbm.at[:, part], hid.at[:, part], hsem.at[p]),
            pltpu.make_async_copy(w_hbm.at[part, pl.ds(0, TILE)], wbuf.at[0, part], fsem.at[p]),
        )

    for p in range(PARTS):
        for copy in first_loads(p):
            copy.start()

    barrier = pltpu.get_barrier_semaphore()

    def knock(d, c):
        pl.semaphore_signal(barrier, inc=1, device_id={"vp": lax.rem(me + d, n)}, device_id_type=MESH)
        return c

    lax.fori_loop(1, n, knock, 0)

    eye = lax.broadcasted_iota(jnp.int32, (LANES, LANES), 0) == lax.broadcasted_iota(jnp.int32, (LANES, LANES), 1)
    shard_start = (me * local_vocab).astype(jnp.float32)
    for q in range(rows // LANES):
        cut = slice(q * LANES, (q + 1) * LANES)
        for src, dst, base in ((inv_ref, invcol, 0.0), (tgt_ref, tcol, shard_start)):
            seg = jnp.broadcast_to(src[cut].reshape(1, LANES).astype(jnp.float32), (LANES, LANES))
            col = jnp.sum(jnp.where(eye, seg, 0.0), axis=1, keepdims=True) - base
            dst[cut, :] = jnp.broadcast_to(col, (LANES, LANES))
    tri[...] = (lax.broadcasted_iota(jnp.int32, (TILE, TILE), 0) <= lax.broadcasted_iota(jnp.int32, (TILE, TILE), 1)).astype(jnp.float32).astype(jnp.bfloat16)
    stat[...] = jnp.zeros_like(stat)

    def columns(t):
        return pl.ds(pl.multiple_of(t * TILE, TILE), TILE)

    def round_columns(r, part):
        if part is None:
            return columns(r), r
        start = (tiles - 1) * TILE + part * HALF
        return pl.ds(start, HALF), tiles - 1 + part

    def first_leg(r, half=None):
        cols, k = round_columns(r, half)
        for hop in (1, side - 1, *range(2, side - 1)):
            to = (a + hop) % side
            pltpu.make_async_remote_copy(
                src_ref=send.at[pl.ds(to * slab, slab), :, cols],
                dst_ref=mid.at[a, :, :, cols],
                send_sem=one_ss,
                recv_sem=one_rs.at[k],
                device_id=device(to, b, core),
                device_id_type=MESH,
            ).start()

    def second_leg(r, half=None):
        cols, k = round_columns(r, half)
        part = mid.at[pl.ds(0, side - 1), :, :, pl.ds(0, TILE if half is None else HALF)]
        pltpu.make_async_copy(part, part, one_rs.at[k]).wait()

        def onward(to, core_):
            pltpu.make_async_remote_copy(
                src_ref=mid.at[:, pl.ds((to * 2 + core_) * own_groups, own_groups), :, cols],
                dst_ref=recv.at[core * side + b, :, :, :, cols],
                send_sem=two_ss,
                recv_sem=two_rs.at[k],
                device_id=device(a, to, core_),
                device_id_type=MESH,
            ).start()

        for hop in (1, side - 1, *range(2, side - 1)):
            for core_ in range(2):
                onward((b + hop) % side, core_)
        onward(b, 1 - core)
        recv[core * side + b, :, :, :, cols] = mid[:, pl.ds((b * 2 + core) * own_groups, own_groups), :, cols]

    def compute_tile(t, send_now=None):
        if send_now:
            z = None
            for p in range(PARTS):
                for copy in first_loads(p):
                    copy.wait()
                if p == PARTS - 1:
                    w_start(jnp.int32(1))
                    w_start(jnp.int32(2))
                term = jnp.dot(hid[:, depth_part(p)], wbuf[0, depth_part(p)], preferred_element_type=jnp.float32)
                z = term if z is None else z + term
        else:
            pltpu.make_async_copy(wbuf.at[t % SLOTS], wbuf.at[t % SLOTS], wsem.at[t % SLOTS]).wait()

            @pl.when(t + 2 < tiles)
            def _():
                w_start(t + 2)

            z = jnp.dot(hid[...], wbuf[t % SLOTS], preferred_element_type=jnp.float32)
        z = z * jnp.concatenate([invcol[...]] * (TILE // LANES), axis=1)
        top = jnp.max(z, axis=1, keepdims=True)
        e = jnp.exp(z - top)
        hi = e.astype(jnp.bfloat16)
        rest = e - hi.astype(jnp.float32)
        more = rest.astype(jnp.bfloat16)
        low = (rest - more.astype(jnp.float32)).astype(jnp.bfloat16)
        upto = tri[...]
        run = jnp.dot(low, upto, preferred_element_type=jnp.float32)
        run = run + jnp.dot(more, upto, preferred_element_type=jnp.float32)
        run = run + jnp.dot(hi, upto, preferred_element_type=jnp.float32)
        cols = columns(t)
        for k in range(rows // SUB):
            owner, g = divmod(k, own_groups)
            oy, ox, oc = owner // (2 * side), (owner // 2) % side, owner % 2
            x_first, y_first = ((ox * side + oy) * 2 + oc) * own_groups + g, ((oy * side + ox) * 2 + oc) * own_groups + g
            send[x_first + core * (y_first - x_first), :, cols] = run[k * SUB : (k + 1) * SUB]
        mid[a, :, :, cols] = send[pl.ds(a * slab, slab), :, cols]
        if send_now:
            send_now()
        at = lax.broadcasted_iota(jnp.int32, (rows, TILE), 1).astype(jnp.float32) + (t * TILE).astype(jnp.float32)
        tc = jnp.concatenate([tcol[...]] * (TILE // LANES), axis=1)
        hit = jnp.sum(jnp.where(at == tc, run, 0.0), axis=1, keepdims=True)
        lane = lax.broadcasted_iota(jnp.int32, (rows, LANES), 1)
        st = stat[...]
        st = jnp.where(lane == t, top, st)
        st = jnp.where(lane == tiles + t, run[:, TILE - 1 :], st)
        st = jnp.where(lane == 2 * tiles, st + hit, st)
        stat[...] = st

    def send_statistics():
        lane8 = lax.broadcasted_iota(jnp.int32, (rows, LANES), 1)
        stat[...] = jnp.where(lane8 == 2 * tiles + 1, tcol[...], stat[...])
        for i in range(n):
            block = None
            for g in range(own_groups):
                k = i * own_groups + g
                part = stat[k * SUB : (k + 1) * SUB, :]
                part = part if g == 0 else pltpu.roll(part, g * width, 1)
                block = part if block is None else block + part
            stat_out[i] = block
        stat_in[me] = stat_out[me]

        def go(d, c):
            peer = lax.rem(me + d, n)
            pltpu.make_async_remote_copy(
                src_ref=stat_out.at[peer], dst_ref=stat_in.at[me], send_sem=stat_ss, recv_sem=stat_rs,
                device_id={"vp": peer}, device_id_type=MESH,
            ).start()
            return c

        lax.fori_loop(1, n, go, 0)

    def take_statistics():
        pltpu.make_async_copy(stat_in.at[pl.ds(0, n - 1)], stat_in.at[pl.ds(0, n - 1)], stat_rs).wait()
        lane = lax.broadcasted_iota(jnp.int32, (n, SUB, LANES), 2)
        first = lane < tiles
        lane4 = lax.broadcasted_iota(jnp.int32, (SUB, LANES), 1)
        row4 = lax.broadcasted_iota(jnp.int32, (SUB, LANES), 0)
        line = jnp.zeros((SUB, LANES), jnp.float32)
        for g in range(own_groups):
            got = stat_in[...]
            if g:
                got = pltpu.roll(got, LANES - g * width, 2)
            tops = jnp.where(first, got, LOW)
            top = jnp.max(jnp.max(tops, axis=0, keepdims=True), axis=2, keepdims=True)
            weight = jnp.where(first, jnp.exp(tops - top), 0.0)
            mass = weight * jnp.where(first, pltpu.roll(got, LANES - tiles, 2), 0.0)
            upto = mass
            shift = 1
            while shift < tiles:
                upto = upto + jnp.where(lane >= shift, pltpu.roll(upto, shift, 2), 0.0)
                shift *= 2
            before = jnp.where(lane >= 1, pltpu.roll(upto, 1, 2), 0.0)
            shard = jnp.sum(mass, axis=2, keepdims=True)
            start = jnp.zeros((1, SUB, 1), jnp.float32)
            starts = []
            for s in range(n):
                starts.append(start)
                start = start + shard[s : s + 1]
            inv = 1.0 / start
            sc = weight * inv
            of = (before + jnp.concatenate(starts, axis=0)) * inv
            scale[g] = sc
            offset[g] = of
            picked = jnp.broadcast_to(got[:, :, 2 * tiles : 2 * tiles + 1], got.shape)
            target = jnp.broadcast_to(got[:, :, 2 * tiles + 1 : 2 * tiles + 2], got.shape)
            lo = (lane * TILE).astype(jnp.float32)
            hit = first & (target >= lo) & (target < lo + float(TILE))
            val = jnp.where(hit, sc * picked + of, 0.0)
            val = jnp.sum(jnp.sum(val, axis=0), axis=1, keepdims=True)
            line = jnp.where(lane4 == row4 + g * SUB, val, line)
        line = jnp.sum(line, axis=0, keepdims=True)
        tval[...] = line
        tall[me] = line

        def go(d, c):
            pltpu.make_async_remote_copy(
                src_ref=tval, dst_ref=tall.at[me], send_sem=t_ss, recv_sem=t_rs,
                device_id={"vp": lax.rem(me + d, n)}, device_id_type=MESH,
            ).start()
            return c

        lax.fori_loop(1, n, go, 0)

    def widen(t):
        for g in range(own_groups):
            for ref, wide in ((scale, scale_b), (offset, offset_b)):
                v = ref[g]
                wide[g] = jnp.broadcast_to(v[:, :, :1], v.shape)
                ref[g] = pltpu.roll(v, LANES - 1, 2)

    def finish_round(r, half=None):
        size = TILE if half is None else HALF
        base = r * TILE if half is None else (tiles - 1) * TILE + half * HALF
        if not half:
            widen(r)
        part = recv.at[pl.ds(0, 2 * side - 1), :, :, :, pl.ds(0, size)]
        pltpu.make_async_copy(part, part, two_rs.at[r if half is None else tiles - 1 + half]).wait()

        def one(q, c):
            relay, u = q // side, q % side
            core_, v = relay // side, relay % side
            row = v + core_ * (u - v)
            col = u + core_ * (v - u)
            s = (row * side + col) * 2 + core_
            for g in range(own_groups):
                sc, of = scale_b[g, s], offset_b[g, s]
                for h in range(size // LANES):
                    here = pl.ds(pl.multiple_of(base + h * LANES, LANES), LANES)
                    cols = pl.ds(pl.multiple_of(s * local_vocab + base + h * LANES, LANES), LANES)
                    out_ref[g * SUB : (g + 1) * SUB, cols] = recv[relay, u, g, :, here] * sc + of
            return c

        lax.fori_loop(0, n, one, 0, unroll=4)

    def first_send():
        pl.semaphore_wait(barrier, n - 1)
        first_leg(jnp.int32(0))

    compute_tile(jnp.int32(0), first_send)

    def early(t, c):
        compute_tile(t)

        @pl.when(t % 2 == 1)
        def _():
            first_leg((t + 1) // 2)

        @pl.when(t % 2 == 0)
        def _():
            second_leg(t // 2 - 1)

        return c

    lax.fori_loop(1, tiles, early, 0)
    send_statistics()

    next_one, next_two = tiles // 2 + 1, tiles // 2 - 1
    first_leg(jnp.int32(next_one))
    lead = next_one + 1 - next_two
    take_at = next_two + 3

    def late(k, c):
        first_leg(k + lead)

        @pl.when(k == take_at)
        def _():
            take_statistics()

        second_leg(k)

        @pl.when(k >= take_at)
        def _():
            for m in range(3):
                finish_round((k - take_at) * 3 + m)

        return c

    stop = tiles - 1 - lead
    lax.fori_loop(next_two, stop, late, 0)
    first_leg(None, 0)
    first_leg(None, 1)

    def finish_to(lo, hi):
        def body(r, c):
            finish_round(r)
            return c

        lax.fori_loop(lo, hi, body, 0)

    def ending(k, c):
        second_leg(k)
        finish_round((k - stop) * 2 + (stop - take_at) * 3)
        finish_round((k - stop) * 2 + (stop - take_at) * 3 + 1)
        return c

    lax.fori_loop(stop, tiles - 1, ending, 0)
    second_leg(None, 0)
    second_leg(None, 1)
    finish_to((stop - take_at) * 3 + lead * 2, tiles - 1)
    pltpu.make_async_copy(tall.at[pl.ds(0, n - 1)], tall.at[pl.ds(0, n - 1)], t_rs).wait()
    own_rows = own_groups * SUB
    lane1 = lax.broadcasted_iota(jnp.int32, (1, LANES), 1)
    acc = [jnp.zeros((1, LANES), jnp.float32) for _ in range(rows // LANES)]
    for s in range(n):
        q, off = divmod(s * own_rows, LANES)
        line = tall[s]
        line = pltpu.roll(line, off, 1) if off else line
        acc[q] = acc[q] + jnp.where(lane1 >= off, line, 0.0)
        if off + own_rows > LANES:
            acc[q + 1] = acc[q + 1] + jnp.where(lane1 < off, line, 0.0)
    for q in range(rows // LANES):
        pick_ref[q * LANES : (q + 1) * LANES] = acc[q].reshape(LANES)

    finish_round(tiles - 1, 0)
    finish_round(tiles - 1, 1)

    pltpu.make_async_copy(mid.at[pl.ds(0, side - 1)], mid.at[pl.ds(0, side - 1)], one_ss).wait()
    pltpu.make_async_copy(recv.at[pl.ds(0, 2 * side - 1)], recv.at[pl.ds(0, 2 * side - 1)], two_ss).wait()
    pltpu.make_async_copy(stat_in.at[pl.ds(0, n - 1)], stat_in.at[pl.ds(0, n - 1)], stat_ss).wait()
    pltpu.make_async_copy(tall.at[pl.ds(0, n - 1)], tall.at[pl.ds(0, n - 1)], t_ss).wait()


def store_kernel(table, picked, table_out, picked_out, sem, small_sem):
    width = table.shape[1] // STORES
    copies = [pltpu.make_async_copy(picked, picked_out, small_sem)]
    for i in range(STORES):
        cols = pl.ds(i * width, width)
        copies.append(pltpu.make_async_copy(table.at[:, cols], table_out.at[:, cols], sem.at[i]))
    for copy in copies:
        copy.start()
    for copy in copies:
        copy.wait()


def solution(mesh):
    n = mesh.shape["vp"]
    side = math.isqrt(n // 2)

    def local_step(hidden, w_local, inv_temp, target_ids):
        rows, depth = hidden.shape
        local_vocab = w_local.shape[1]
        tiles = local_vocab // TILE
        groups = rows // SUB
        own_rows = rows // n
        f32 = jnp.float32
        table, picked = pl.pallas_call(
            functools.partial(kernel, n),
            out_shape=(
                pltpu.VMEM((own_rows, n * local_vocab), f32),
                pltpu.VMEM((rows,), f32),
            ),
            in_specs=[
                pl.BlockSpec(memory_space=pltpu.HBM),
                pl.BlockSpec(memory_space=pltpu.HBM),
                pl.BlockSpec(memory_space=pltpu.VMEM),
                pl.BlockSpec(memory_space=pltpu.VMEM),
            ],
            out_specs=(pl.BlockSpec(memory_space=pltpu.VMEM), pl.BlockSpec(memory_space=pltpu.VMEM)),
            scratch_shapes=[
                pltpu.VMEM((rows, depth), jnp.bfloat16),
                pltpu.VMEM((SLOTS, depth, TILE), jnp.bfloat16),
                pltpu.VMEM((groups, SUB, local_vocab), f32),
                pltpu.VMEM((side, groups // side, SUB, local_vocab), f32),
                pltpu.VMEM((2 * side, side, own_rows // SUB, SUB, local_vocab), f32),
                pltpu.VMEM((rows, LANES), f32),
                pltpu.VMEM((rows, LANES), f32),
                pltpu.VMEM((TILE, TILE), jnp.bfloat16),
                pltpu.VMEM((rows, LANES), f32),
                pltpu.VMEM((n, SUB, LANES), f32),
                pltpu.VMEM((n, SUB, LANES), f32),
                pltpu.VMEM((own_rows // SUB, n, SUB, LANES), f32),
                pltpu.VMEM((own_rows // SUB, n, SUB, LANES), f32),
                pltpu.VMEM((own_rows // SUB, n, SUB, LANES), f32),
                pltpu.VMEM((own_rows // SUB, n, SUB, LANES), f32),
                pltpu.VMEM((1, LANES), f32),
                pltpu.VMEM((n, 1, LANES), f32),
                pltpu.SemaphoreType.DMA((PARTS,)),
                pltpu.SemaphoreType.DMA((PARTS,)),
                pltpu.SemaphoreType.DMA((SLOTS,)),
                pltpu.SemaphoreType.DMA,
                pltpu.SemaphoreType.DMA((tiles + 1,)),
                pltpu.SemaphoreType.DMA,
                pltpu.SemaphoreType.DMA((tiles + 1,)),
                pltpu.SemaphoreType.DMA,
                pltpu.SemaphoreType.DMA,
                pltpu.SemaphoreType.DMA,
                pltpu.SemaphoreType.DMA,
            ],
            compiler_params=pltpu.CompilerParams(collective_id=0, has_side_effects=True, vmem_limit_bytes=54 << 20),
            name="head_cdf",
        )(hidden, w_local, inv_temp, target_ids)
        return pl.pallas_call(
            store_kernel,
            out_shape=(
                jax.ShapeDtypeStruct(table.shape, f32),
                jax.ShapeDtypeStruct(picked.shape, f32),
            ),
            in_specs=[pl.BlockSpec(memory_space=pltpu.VMEM)] * 2,
            out_specs=(pl.BlockSpec(memory_space=pltpu.HBM), pl.BlockSpec(memory_space=pltpu.HBM)),
            scratch_shapes=[pltpu.SemaphoreType.DMA((STORES,)), pltpu.SemaphoreType.DMA],
            compiler_params=pltpu.CompilerParams(vmem_limit_bytes=20 << 20),
            name="store_table",
        )(table, picked)

    return jax.shard_map(
        local_step,
        mesh=mesh,
        in_specs=(P("dp", None), P(None, "vp"), P("dp"), P("dp")),
        out_specs=(P(("dp", "vp"), None), P("dp")),
        check_vma=False,
    )
```
